32 devices in a mesh: sample: 2 (over x), fsdp: 4 (over z), seq: 4 (over y, core).
Axes of the slice: x: 2, y: 2, z: 4, core: 2. Of those that a mesh axis runs over, the one named last changes fastest.
Arguments:
- token_act: bfloat16 [8, 512, 768], P(('sample', 'fsdp'), 'seq'), may hold values from -40 to 40
- token_cond: bfloat16 [8, 512, 768], P(('sample', 'fsdp'), 'seq'), may hold values from -40 to 40
- pair_bias: bfloat16 [16, 512, 512], P('fsdp', 'seq'), may hold values from -8 to 296
- token_mask: int32 [512], P('seq'), may hold values 0 or 1
- ada_weights: bfloat16 [4, 768, 768], P(None, None, 'fsdp'), may hold values from -0.21875 to 0.21875
- attention_in: bfloat16 [4, 768, 768], P(None, None, 'fsdp'), may hold values from -0.21875 to 0.21875
- attention_out: bfloat16 [768, 768], P('fsdp'), may hold values from -0.21875 to 0.21875
- transition_in: bfloat16 [2, 768, 1536], P(None, None, 'fsdp'), may hold values from -0.21875 to 0.21875
- transition_out: bfloat16 [1536, 768], P('fsdp'), may hold values from -0.15625 to 0.15625
- token_vectors: float32 [3, 768], replicated, may hold values from -4 to 4
- atom_skip: bfloat16 [8, 4096, 128], P(('sample', 'fsdp'), 'seq'), may hold values from -40 to 40
- atom_cond: bfloat16 [4096, 128], P('seq'), may hold values from -40 to 40
- atom_bias: bfloat16 [4, 4096, 128], P(None, 'seq'), may hold values from -6 to 296
- window_bounds: int32 [128, 2], P('seq'), may hold values from 0 to 4096, as said below
- atom_token: int32 [4096], P('seq'), may hold values from 0 to 511, as said below
- atom_weights: bfloat16 [7, 128, 128], P(None, None, 'fsdp'), may hold values from -0.5 to 0.5
- token_to_atom: bfloat16 [768, 128], P('fsdp'), may hold values from -0.21875 to 0.21875
- atom_vectors: float32 [2, 128], replicated, may hold values from -4 to 4
- position_out: bfloat16 [3, 128], replicated, may hold values from -0.5 to 0.5
Outputs:
- token_out: bfloat16 [8, 512, 768], P(('sample', 'fsdp'), 'seq')
- position_update: float32 [8, 3, 4096], P(('sample', 'fsdp'), None, 'seq')
The draws below stay inside these ranges and needn't reach their ends.
Inputs may be any that keep to these rules, and one draw needn't show every extreme that they name: `window_bounds`: row b belongs to the atoms 32 * b to 32 * b + 31; column 0 is at least 0 and at least 32 * b - 48, and at most 32 * b; column 1 is at least 32 * b + 32, at most 32 * b + 80 and at most 4096. `atom_token`: atoms are numbered in token order: the value never falls from one atom to the next, the first atom belongs to token 0, the last to token 511, and every token owns 1 to 24 atoms.
All inputs are finite; a program needn't handle non-finite values. No bound on the sum of `token_mask` on one device may be relied on, other than what follows from the above.
Results may differ from the reference program's by a relative error of at most 0.014.
Values may be sent and summed in bfloat16 or wider, within the bound.
A program may use at most 128 MiB of HBM per device.

```python
import math
import jax
import jax.numpy as jnp
from jax import lax

D = 768
H = 16
FF = 1536
CA = 128
HA = 4
WQ = 32
WK = 128
TOKENS = 512
ATOMS = 4096
BLOCKS = 128
SAMPLES = 8
HD = 48


def feature_draw(key, shape):
    base = jnp.clip(jax.random.normal(jax.random.fold_in(key, 11), shape, jnp.float32), -4.0, 4.0)
    return base.astype(jnp.bfloat16)


def draw_token_act(key, part):
    return feature_draw(jax.random.fold_in(key, 101), (SAMPLES, TOKENS, D))


def draw_token_cond(key, part):
    return feature_draw(jax.random.fold_in(key, 102), (SAMPLES, TOKENS, D))


def draw_atom_skip(key, part):
    return feature_draw(jax.random.fold_in(key, 103), (SAMPLES, ATOMS, CA))


def draw_atom_cond(key, part):
    return feature_draw(jax.random.fold_in(key, 104), (ATOMS, CA))


def draw_pair_bias(key, part):
    key = jax.random.fold_in(key, 301)
    values = jnp.clip(2.0 * jax.random.normal(jax.random.fold_in(key, 1), (H, TOKENS, TOKENS), jnp.float32), -8.0, 8.0)
    return values.astype(jnp.bfloat16)


def draw_atom_bias(key, part):
    key = jax.random.fold_in(key, 401)
    values = jnp.clip(1.5 * jax.random.normal(jax.random.fold_in(key, 1), (HA, ATOMS, WK), jnp.float32), -6.0, 6.0)
    return values.astype(jnp.bfloat16)


def draw_window_bounds(key, part):
    key = jax.random.fold_in(key, 501)
    rim_width = (WK - WQ) // 2
    block_start = WQ * jnp.arange(BLOCKS, dtype=jnp.int32)
    lower_end = jnp.maximum(block_start - jax.random.randint(jax.random.fold_in(key, 1), (BLOCKS,), 0, rim_width + 1), 0)
    upper_end = jnp.minimum(block_start + WQ + jax.random.randint(jax.random.fold_in(key, 2), (BLOCKS,), 0, rim_width + 1), ATOMS)
    return jnp.stack([lower_end, upper_end], axis=1).astype(jnp.int32)


def paired_runs(key, pair_count, pair_total):
    first = jax.random.randint(key, (pair_count,), 1, pair_total)
    return jnp.stack([first, pair_total - first], axis=1).reshape(-1).astype(jnp.int32)


def draw_atom_token(key, part):
    key = jax.random.fold_in(key, 601)
    quarter = TOKENS // 4
    group_size = TOKENS // 16
    long_runs = jnp.full((quarter,), 24, jnp.int32)
    middle_runs = paired_runs(jax.random.fold_in(key, 1), quarter // 2, 8)
    short_runs = paired_runs(jax.random.fold_in(key, 2), quarter, 4)
    lengths = jnp.concatenate([long_runs, middle_runs, short_runs]).astype(jnp.int32)
    rest_order = jax.random.permutation(jax.random.fold_in(key, 3), 12).astype(jnp.int32) + 4
    order = jnp.concatenate([jnp.arange(4, dtype=jnp.int32), rest_order]).astype(jnp.int32)
    lengths = jnp.take(lengths.reshape(16, group_size), order, axis=0).reshape(-1).astype(jnp.int32)
    run_ends = jnp.cumsum(lengths)
    marks = jnp.zeros((ATOMS,), jnp.int32).at[run_ends[:-1]].add(1)
    return jnp.cumsum(marks).astype(jnp.int32)


def place_ends(drawn, key, smallest, largest):
    longest = drawn.shape.index(max(drawn.shape))
    spots = []
    for shift in (0, 1):
        where = [jax.random.randint(jax.random.fold_in(key, axis), (), 0, length) for axis, length in enumerate(drawn.shape)]
        where[longest] = (where[longest] + shift) % drawn.shape[longest]
        spots.append(tuple(where))
    return drawn.at[spots[0]].set(smallest).at[spots[1]].set(largest)


def steps_of(key, dims, split, low, largest):
    def one(dim, shards_of):
        steps = jax.random.uniform(jax.random.fold_in(jax.random.fold_in(key, 6), dim), (shards_of,), jnp.float32, low / len(split), largest / len(split))
        return jnp.repeat(jnp.exp(steps), dims[dim] // shards_of).reshape((-1,) + (1,) * (len(dims) - dim - 1))

    loudness = one(*split[0])
    for cut in split[1:]:
        loudness = loudness * one(*cut)
    return loudness


def bell_draw(stream_key, shape, scale, limit, shards=(), kind=jnp.bfloat16):
    values = jax.random.normal(stream_key, shape, jnp.float32) * scale
    if len(shards) > 0:
        values = steps_of(stream_key, shape, shards, -0.22, 0.18) * values
    return jnp.clip(values, min=-limit, max=limit).astype(kind)


def setup_inputs(seed: int = 0) -> dict:
    arg_keys = jax.random.split(jax.random.key(seed), 20)
    token_act = draw_token_act(jax.random.fold_in(arg_keys[19], 71), 0)
    token_cond = draw_token_cond(jax.random.fold_in(arg_keys[19], 71), 0)
    pair_bias = draw_pair_bias(jax.random.fold_in(arg_keys[19], 71), 0)
    token_mask = place_ends((jax.random.randint(arg_keys[3], (TOKENS,), 0, 8) < 7).astype(jnp.int32), jax.random.fold_in(arg_keys[3], 1), 0, 1)
    ada_weights = bell_draw(arg_keys[4], (4, D, D), D ** -0.5, 0.21875, ((2, 4),))
    attention_in = bell_draw(arg_keys[5], (4, D, D), D ** -0.5, 0.21875, ((2, 4),))
    attention_out = bell_draw(arg_keys[6], (D, D), D ** -0.5, 0.21875, ((0, 4),))
    transition_in = bell_draw(arg_keys[7], (2, D, FF), D ** -0.5, 0.21875, ((2, 4),))
    transition_out = bell_draw(arg_keys[8], (FF, D), FF ** -0.5, 0.15625, ((0, 4),))
    token_vectors = bell_draw(arg_keys[9], (3, D), 1.0, 4.0, (), jnp.float32)
    atom_skip = draw_atom_skip(jax.random.fold_in(arg_keys[19], 71), 0)
    atom_cond = draw_atom_cond(jax.random.fold_in(arg_keys[19], 71), 0)
    atom_bias = draw_atom_bias(jax.random.fold_in(arg_keys[19], 71), 0)
    window_bounds = draw_window_bounds(jax.random.fold_in(arg_keys[19], 71), 0)
    atom_token = draw_atom_token(jax.random.fold_in(arg_keys[19], 71), 0)
    atom_weights = bell_draw(arg_keys[15], (7, CA, CA), CA ** -0.5, 0.5, ((2, 4),))
    token_to_atom = bell_draw(arg_keys[16], (D, CA), D ** -0.5, 0.21875, ((0, 4),))
    atom_vectors = bell_draw(arg_keys[17], (2, CA), 1.0, 4.0, (), jnp.float32)
    position_out = bell_draw(arg_keys[18], (3, CA), CA ** -0.5, 0.5)
    return {"token_act": token_act, "token_cond": token_cond, "pair_bias": pair_bias, "token_mask": token_mask, "ada_weights": ada_weights, "attention_in": attention_in, "attention_out": attention_out, "transition_in": transition_in, "transition_out": transition_out, "token_vectors": token_vectors, "atom_skip": atom_skip, "atom_cond": atom_cond, "atom_bias": atom_bias, "window_bounds": window_bounds, "atom_token": atom_token, "atom_weights": atom_weights, "token_to_atom": token_to_atom, "atom_vectors": atom_vectors, "position_out": position_out}


EPS = 1e-05
FAR = -1e+30

def layer_norm(values):
    values = values.astype(jnp.float32)
    center = values - lax.optimization_barrier(jnp.mean(values, axis=-1, keepdims=True))
    spread = lax.optimization_barrier(jnp.mean(center * center, axis=-1, keepdims=True))
    return center * lax.rsqrt(spread + EPS)

def matmul(left_side, right_side):
    return jnp.dot(left_side, right_side, preferred_element_type=jnp.float32)

def adaptive(values, normed_cond, scale_weight, shift_weight, offset):
    return jax.nn.sigmoid(matmul(normed_cond, scale_weight) + offset) * layer_norm(values) + matmul(normed_cond, shift_weight)

def window_attention(queries, pairs, bias_rows, bounds):
    atom_count, feature_count = queries.shape
    block_count = atom_count // WQ
    step_count = WK // WQ
    rim_width = (WK - WQ) // 2
    head_width = feature_count // HA
    padded = jnp.pad(pairs, ((rim_width, rim_width), (0, 0)))
    tile_rows = padded.reshape(block_count + step_count - 1, WQ, 2 * feature_count)
    windows = jnp.concatenate([tile_rows[position:position + block_count] for position in range(step_count)], axis=1)
    key_rows = windows[:, :, :feature_count].reshape(block_count, WK, HA, head_width)
    value_rows = windows[:, :, feature_count:].reshape(block_count, WK, HA, head_width)
    query_rows = queries.reshape(block_count, WQ, HA, head_width)
    scores = jnp.einsum('bqhd,bkhd->hbqk', query_rows.astype(jnp.float32), key_rows.astype(jnp.float32)) * (1.0 / math.sqrt(head_width))
    scores = scores + bias_rows.reshape(HA, block_count, WQ, WK).astype(jnp.float32)
    slot_atoms = WQ * jnp.arange(block_count, dtype=jnp.int32)[:, None] - rim_width + jnp.arange(WK, dtype=jnp.int32)[None, :]
    in_window = (slot_atoms >= bounds[:, 0:1]) & (slot_atoms < bounds[:, 1:2])
    scores = jnp.where(in_window[None, :, None, :], scores, FAR)
    maxima = lax.optimization_barrier(jnp.max(scores, axis=-1, keepdims=True))
    weights = jnp.exp(scores - maxima)
    totals = lax.optimization_barrier(jnp.sum(weights, axis=-1))
    attended = jnp.einsum('hbqk,bkhd->bqhd', weights.astype(jnp.bfloat16).astype(jnp.float32), value_rows.astype(jnp.float32))
    attended = attended / jnp.transpose(totals, (1, 2, 0))[..., None]
    return attended.reshape(atom_count, feature_count)

def reference(token_act, token_cond, pair_bias, token_mask, ada_weights, attention_in, attention_out, transition_in, transition_out, token_vectors, atom_skip, atom_cond, atom_bias, window_bounds, atom_token, atom_weights, token_to_atom, atom_vectors, position_out):
    cond_normed = layer_norm(token_cond).astype(jnp.bfloat16)
    attend_x = adaptive(token_act, cond_normed, ada_weights[0], ada_weights[1], token_vectors[0]).astype(jnp.bfloat16)
    transit_x = adaptive(token_act, cond_normed, ada_weights[2], ada_weights[3], token_vectors[1]).astype(jnp.bfloat16)
    query_rows = (matmul(attend_x, attention_in[0]) + token_vectors[2]).astype(jnp.bfloat16)
    key_rows = matmul(attend_x, attention_in[1]).astype(jnp.bfloat16)
    value_rows = matmul(attend_x, attention_in[2]).astype(jnp.bfloat16)
    gate_rows = matmul(attend_x, attention_in[3]).astype(jnp.bfloat16)
    query_heads = query_rows.reshape(SAMPLES, TOKENS, H, HD)
    key_heads = key_rows.reshape(SAMPLES, TOKENS, H, HD)
    value_heads = value_rows.reshape(SAMPLES, TOKENS, H, HD)
    live_keys = token_mask > 0
    score_scale = 1.0 / math.sqrt(HD)

    def one_head(combined):
        sample = (combined // H).astype(jnp.int32)
        head_id = (combined % H).astype(jnp.int32)
        query_one = lax.dynamic_index_in_dim(lax.dynamic_index_in_dim(query_heads, sample, 0, False), head_id, 1, False)
        key_one = lax.dynamic_index_in_dim(lax.dynamic_index_in_dim(key_heads, sample, 0, False), head_id, 1, False)
        value_one = lax.dynamic_index_in_dim(lax.dynamic_index_in_dim(value_heads, sample, 0, False), head_id, 1, False)
        bias_one = lax.dynamic_index_in_dim(pair_bias, head_id, 0, False).astype(jnp.float32)
        scores = jnp.dot(query_one, key_one.T, preferred_element_type=jnp.float32) * score_scale + bias_one
        scores = jnp.where(live_keys[None, :], scores, FAR)
        maxima = lax.optimization_barrier(jnp.max(scores, axis=-1, keepdims=True))
        weights = jnp.exp(scores - maxima)
        totals = lax.optimization_barrier(jnp.sum(weights, axis=-1, keepdims=True))
        return matmul(weights.astype(jnp.bfloat16), value_one) / totals
    head_outputs = lax.map(one_head, jnp.arange(SAMPLES * H, dtype=jnp.int32))
    attended = head_outputs.reshape(SAMPLES, H, TOKENS, HD).transpose(0, 2, 1, 3).reshape(SAMPLES, TOKENS, D)
    gated = (attended * jax.nn.sigmoid(gate_rows.astype(jnp.float32))).astype(jnp.bfloat16)
    hidden = (jax.nn.silu(matmul(transit_x, transition_in[0])) * matmul(transit_x, transition_in[1])).astype(jnp.bfloat16)
    token_out = (token_act.astype(jnp.float32) + matmul(gated, attention_out) + matmul(hidden, transition_out)).astype(jnp.bfloat16)
    token_rows = matmul(token_out, token_to_atom).astype(jnp.bfloat16)
    atom_state = atom_skip.astype(jnp.float32) + jnp.take(token_rows, atom_token, axis=1).astype(jnp.float32)
    atom_normed = layer_norm(atom_cond).astype(jnp.bfloat16)
    atom_x = adaptive(atom_state, atom_normed, atom_weights[0], atom_weights[1], atom_vectors[0]).astype(jnp.bfloat16)
    atom_query = (matmul(atom_x, atom_weights[2]) + atom_vectors[1]).astype(jnp.bfloat16)
    atom_key = matmul(atom_x, atom_weights[3]).astype(jnp.bfloat16)
    atom_value = matmul(atom_x, atom_weights[4]).astype(jnp.bfloat16)
    atom_gate = matmul(atom_x, atom_weights[5]).astype(jnp.bfloat16)
    pairs = jnp.concatenate([atom_key, atom_value], axis=-1)

    def one_sample(operands):
        return window_attention(operands[0], operands[1], atom_bias, window_bounds)
    atom_attended = lax.map(one_sample, (atom_query, pairs))
    atom_gated = (atom_attended * jax.nn.sigmoid(atom_gate.astype(jnp.float32))).astype(jnp.bfloat16)
    atom_new = atom_state + matmul(atom_gated, atom_weights[6])
    final_normed = layer_norm(atom_new).astype(jnp.bfloat16)
    position_update = jnp.einsum('ck,sak->sca', position_out.astype(jnp.float32), final_normed.astype(jnp.float32))
    return (token_out, position_update)
```

```python
import functools
import math

import jax
import jax.numpy as jnp
from jax import lax
from jax.experimental import pallas as pl
from jax.experimental.pallas import tpu as pltpu
from jax.sharding import PartitionSpec as P

HA = 4
WQ = 32
WK = 128
HD = 48
EPS = 1e-05
FAR = -1e30
RIM = (WK - WQ) // 2
VMEM_LIMIT = 56 * 1024 * 1024
MESH = pl.DeviceIdType.MESH


def layer_norm(values):
    values = values.astype(jnp.float32)
    center = values - jnp.mean(values, axis=-1, keepdims=True)
    spread = jnp.mean(center * center, axis=-1, keepdims=True)
    return center * lax.rsqrt(spread + EPS)


def matmul(left_side, right_side):
    return jnp.dot(left_side, right_side, preferred_element_type=jnp.float32)


def pack(array):
    half = array.shape[-2] // 2
    return jnp.concatenate([array[..., :half, :], array[..., half:, :]], axis=-1)


def unpack(array):
    half = array.shape[-1] // 2
    return jnp.concatenate([array[..., :half], array[..., half:]], axis=-2)


class Line:
    def __init__(self, axis, size, paired, block, out, send, recv, local, partner_send, partner_recv):
        self.axis, self.size, self.paired = axis, size, paired
        self.block, self.out, self.send, self.recv, self.local = block, out, send, recv, local
        self.partner_send, self.partner_recv = partner_send, partner_recv
        self.index = lax.axis_index(axis)
        self.stride = 2 if paired else 1
        self.length = size // self.stride
        self.position = self.index // 2 if paired else self.index
        self.parity = self.index - 2 * self.position if paired else 0

    def slot(self, position):
        return position * self.stride + self.parity

    def partner(self):
        return self.index + 1 - 2 * self.parity

    def guards(self, side, step):
        here, last = self.position, self.length - 1
        if side == 0:
            return (here - step >= 0) & (here < last), here - 1 - step >= 0
        return (here + step <= last) & (here > 0), here + 1 + step <= last

    def copy(self, side, step, arriving):
        sign = 1 if side == 0 else -1
        origin = self.position - sign * (step + (1 if arriving else 0))
        target = self.slot(self.position + sign)
        slot = self.slot(origin)
        source = self.block if (step == 0 and not arriving) else self.out.at[slot]
        return pltpu.make_async_remote_copy(
            src_ref=source,
            dst_ref=self.out.at[slot],
            send_sem=self.send.at[side, step],
            recv_sem=self.recv.at[side, step],
            device_id={self.axis: target},
            device_id_type=MESH,
        )

    def hand(self, key, origin, own, arriving):
        slot = self.slot(origin)
        landing = origin * 2 + 1 - self.parity if arriving else slot
        return pltpu.make_async_remote_copy(
            src_ref=self.block if own else self.out.at[slot],
            dst_ref=self.out.at[landing],
            send_sem=self.partner_send.at[key],
            recv_sem=self.partner_recv.at[key],
            device_id={self.axis: self.partner()},
            device_id_type=MESH,
        )

    def greet(self, barrier):
        def neighbour(target):
            pl.semaphore_signal(barrier, inc=1, device_id={self.axis: target}, device_id_type=MESH)

        expected = 0
        if self.length > 1:
            above = self.position > 0
            below = self.position < self.length - 1

            @pl.when(above)
            def _():
                neighbour(self.slot(self.position - 1))

            @pl.when(below)
            def _():
                neighbour(self.slot(self.position + 1))

            expected = jnp.where(above, 1, 0) + jnp.where(below, 1, 0)
        if self.paired:
            neighbour(self.partner())
            expected = expected + 1
        return expected

    def begin(self):
        pltpu.make_async_copy(self.block, self.out.at[self.index], self.local.at[0]).start()
        if self.paired:
            self.hand(0, self.position, True, False).start()

    def advance(self, step):
        for side in (0, 1):
            goes, unused = self.guards(side, step)
            if step > 0:
                self.arrive(side, step - 1)

            @pl.when(goes)
            def _():
                self.copy(side, step, False).start()

    def arrive(self, side, step):
        unused, comes = self.guards(side, step)

        @pl.when(comes)
        def _():
            self.copy(side, step, True).wait_recv()
            if self.paired:
                origin = self.position - (step + 1) if side == 0 else self.position + step + 1
                self.hand(1 + side * (self.length - 1) + step, origin, False, False).start()

    def steps(self):
        return self.length - 1

    def finish(self):
        last = self.length - 1
        if last > 0:
            for side in (0, 1):
                self.arrive(side, last - 1)
        for side in (0, 1):
            for step in range(last):
                goes, comes = self.guards(side, step)

                @pl.when(goes)
                def _():
                    self.copy(side, step, False).wait_send()

                if self.paired:

                    @pl.when(comes)
                    def _():
                        origin = self.position - (step + 1) if side == 0 else self.position + step + 1
                        key = 1 + side * last + step
                        self.hand(key, origin, False, False).wait_send()
                        self.hand(key, origin, False, True).wait_recv()

        if self.paired:
            self.hand(0, self.position, True, False).wait_send()
            self.hand(0, self.position, True, True).wait_recv()
        pltpu.make_async_copy(self.block, self.out.at[self.index], self.local.at[0]).wait()


class Exchange:
    def __init__(self, axis, size, block, out, send, recv, local):
        self.axis, self.size, self.block, self.out = axis, size, block, out
        self.send, self.recv, self.local = send, recv, local
        self.index = lax.axis_index(axis)

    def peer(self, shift):
        return lax.rem(self.index + shift, self.size)

    def greet(self, barrier):
        for shift in range(1, self.size):
            pl.semaphore_signal(
                barrier, inc=1, device_id={self.axis: self.peer(shift)}, device_id_type=MESH
            )
        return self.size - 1

    def copy(self, shift, arriving):
        landing = self.peer(self.size - shift) if arriving else self.index
        return pltpu.make_async_remote_copy(
            src_ref=self.block.at[self.peer(shift)],
            dst_ref=self.out.at[landing],
            send_sem=self.send.at[shift],
            recv_sem=self.recv.at[shift],
            device_id={self.axis: self.peer(shift)},
            device_id_type=MESH,
        )

    def begin(self):
        pltpu.make_async_copy(
            self.block.at[self.index], self.out.at[self.index], self.local.at[0]
        ).start()
        for shift in range(1, self.size):
            self.copy(shift, False).start()

    def steps(self):
        return 0

    def advance(self, step):
        pass

    def finish(self):
        for shift in range(1, self.size):
            self.copy(shift, False).wait_send()
            self.copy(shift, True).wait_recv()
        pltpu.make_async_copy(
            self.block.at[self.index], self.out.at[self.index], self.local.at[0]
        ).wait()


def move_kernel(kinds, *refs):
    count = len(kinds)
    blocks, outs, sems = refs[:count], refs[count : 2 * count], refs[2 * count :]
    flows, taken = [], 0
    for (kind, axis, size), block, out in zip(kinds, blocks, outs):
        if kind == "exchange":
            flows.append(Exchange(axis, size, block, out, *sems[taken : taken + 3]))
            taken += 3
        elif kind == "paired":
            flows.append(Line(axis, size, True, block, out, *sems[taken : taken + 5]))
            taken += 5
        else:
            flows.append(Line(axis, size, False, block, out, *sems[taken : taken + 3], None, None))
            taken += 3
    barrier = pltpu.get_barrier_semaphore()
    groups, seen = [], set()
    for (kind, axis, size), flow in zip(kinds, flows):
        if axis in seen:
            continue
        wide = [f for (k, a, s), f in zip(kinds, flows) if a == axis and k == "exchange"]
        groups.append(wide[0] if wide else flow)
        seen.add(axis)
    expected = 0
    for group in groups:
        expected = expected + group.greet(barrier)
    pl.semaphore_wait(barrier, expected)
    for flow in flows:
        flow.begin()
    for step in range(max(flow.steps() for flow in flows)):
        for flow in flows:
            if step < flow.steps():
                flow.advance(step)
    for flow in flows:
        flow.finish()


def move(identity, items):
    kinds, arrays, shapes, scratch = [], [], [], []
    sent = 0
    for kind, axis, array in items:
        size = lax.axis_size(axis)
        kinds.append((kind, axis, size))
        arrays.append(array)
        shape = array.shape if kind == "exchange" else (size,) + array.shape
        shapes.append(jax.ShapeDtypeStruct(shape, array.dtype))
        sent += array.size * array.dtype.itemsize
        dma = pltpu.SemaphoreType.DMA
        if kind == "exchange":
            scratch += [dma((size,)), dma((size,)), dma((1,))]
        else:
            length = size // 2 if kind == "paired" else size
            steps = max(length - 1, 1)
            scratch += [dma((2, steps)), dma((2, steps)), dma((1,))]
            if kind == "paired":
                scratch += [dma((2 * length,)), dma((2 * length,))]
    return pl.pallas_call(
        functools.partial(move_kernel, tuple(kinds)),
        out_shape=tuple(shapes),
        in_specs=[pl.BlockSpec(memory_space=pltpu.VMEM)] * len(arrays),
        out_specs=tuple([pl.BlockSpec(memory_space=pltpu.VMEM)] * len(arrays)),
        scratch_shapes=scratch,
        compiler_params=pltpu.CompilerParams(
            collective_id=identity, has_side_effects=True, vmem_limit_bytes=VMEM_LIMIT
        ),
        cost_estimate=pl.CostEstimate(flops=0, bytes_accessed=30 * sent, transcendentals=0),
        name=f"move{identity}",
    )(*arrays)


def attention_kernel(heads, span, q_ref, gate_ref, kv_ref, bias_ref, mask_ref, out_ref):
    rows, width = q_ref.shape[1], q_ref.shape[2]
    pieces, piece_rows = kv_ref.shape[0], kv_ref.shape[2]
    queries = q_ref[0]
    head_of = lax.broadcasted_iota(jnp.int32, (rows, width), 1) // HD
    stacked = jnp.concatenate(
        [jnp.where(head_of == head, queries, 0).astype(jnp.bfloat16) for head in range(heads)], axis=0
    )
    scale = 1.0 / math.sqrt(HD)
    maxima = totals = summed = None
    for first in range(0, pieces, span):
        taken = min(span, pieces - first)
        keys = jnp.concatenate([kv_ref[first + i, 0, :, :width] for i in range(taken)], axis=0)
        values = jnp.concatenate([kv_ref[first + i, 0, :, width:] for i in range(taken)], axis=0)
        columns = pl.ds(first * piece_rows, taken * piece_rows)
        scores = (
            lax.dot_general(
                stacked, keys, (((1,), (1,)), ((), ())), preferred_element_type=jnp.float32
            )
            * scale
        )
        bias = bias_ref[:, :, columns].reshape(heads * rows, taken * piece_rows)
        scores = scores + bias.astype(jnp.float32)
        scores = jnp.where(mask_ref[:, columns] > 0, scores, FAR)
        block_max = jnp.max(scores, axis=-1, keepdims=True)
        new_maxima = block_max if maxima is None else jnp.maximum(maxima, block_max)
        weights = jnp.exp(scores - new_maxima)
        block_total = jnp.sum(weights, axis=-1, keepdims=True)
        update = matmul(weights.astype(jnp.bfloat16), values)
        if maxima is None:
            totals, summed = block_total, update
        else:
            factor = jnp.exp(maxima - new_maxima)
            totals = totals * factor + block_total
            summed = summed * factor + update
        maxima = new_maxima
    attended = summed / totals
    result = jnp.zeros((rows, width), jnp.float32)
    for head in range(heads):
        result = result + jnp.where(head_of == head, attended[head * rows : (head + 1) * rows], 0.0)
    gate = jax.nn.sigmoid(gate_ref[0].astype(jnp.float32))
    out_ref[0] = (result * gate).astype(jnp.bfloat16)


def token_attention(query_rows, gate_rows, kv_all, pair_bias, mask_row):
    groups, rows, width = query_rows.shape
    heads, keys = pair_bias.shape[0], pair_bias.shape[2]
    pieces, piece_rows = kv_all.shape[0], kv_all.shape[2]
    one = lambda g: (g, 0, 0)
    return pl.pallas_call(
        functools.partial(attention_kernel, heads, max(512 // piece_rows, 1)),
        grid=(groups,),
        in_specs=[
            pl.BlockSpec((1, rows, width), one),
            pl.BlockSpec((1, rows, width), one),
            pl.BlockSpec((pieces, 1, piece_rows, 2 * width), lambda g: (0, g, 0, 0)),
            pl.BlockSpec((heads, rows, keys), lambda g: (0, 0, 0)),
            pl.BlockSpec((1, keys), lambda g: (0, 0)),
        ],
        out_specs=pl.BlockSpec((1, rows, width), one),
        out_shape=jax.ShapeDtypeStruct((groups, rows, width), jnp.bfloat16),
        compiler_params=pltpu.CompilerParams(vmem_limit_bytes=VMEM_LIMIT),
        name="token_attention",
    )(query_rows, gate_rows, kv_all, pair_bias, mask_row)


def atom_kernel(
    first_ref, bounds_ref, rows_ref, skip_ref, cond_ref, token_ref, weight_ref, vector_ref,
    position_ref, bias_ref, out_ref, state_ref, query_ref, gate_ref, key_ref, value_ref, held_ref,
):
    count, channels = query_ref.shape
    head_width = channels // HA
    tokens = rows_ref.shape[0]
    chunk = min(512, tokens)
    inner = pl.ds(RIM, count)
    owners = token_ref[...]
    taken = jnp.zeros((owners.shape[0], channels), jnp.float32)
    for start in range(0, tokens, chunk):
        column = lax.broadcasted_iota(jnp.int32, (owners.shape[0], chunk), 1) + start
        hit = jnp.where(owners == column, 1.0, 0.0).astype(jnp.bfloat16)
        taken = taken + matmul(hit, rows_ref[start : start + chunk, :])
    state = skip_ref[...].astype(jnp.float32) + taken
    state_ref[...] = state
    normed = layer_norm(cond_ref[...]).astype(jnp.bfloat16)
    atom_x = (
        jax.nn.sigmoid(matmul(normed, weight_ref[0]) + vector_ref[0:1, :]) * layer_norm(state)
        + matmul(normed, weight_ref[1])
    ).astype(jnp.bfloat16)
    own_x = atom_x[RIM : RIM + count, :]
    query_ref[...] = (matmul(own_x, weight_ref[2]) + vector_ref[1:2, :]).astype(jnp.bfloat16)
    gate_ref[...] = matmul(own_x, weight_ref[5]).astype(jnp.bfloat16)
    key_ref[...] = matmul(atom_x, weight_ref[3]).astype(jnp.bfloat16)
    value_ref[...] = matmul(atom_x, weight_ref[4]).astype(jnp.bfloat16)
    head_of = lax.broadcasted_iota(jnp.int32, (WQ, channels), 1) // head_width
    lane = lax.broadcasted_iota(jnp.int32, (1, WK), 1)
    scale = 1.0 / math.sqrt(head_width)

    def window(index, carry):
        base = pl.multiple_of(index * WQ, WQ)
        queries = query_ref[pl.ds(base, WQ), :]
        stacked = jnp.concatenate(
            [jnp.where(head_of == head, queries, 0).astype(jnp.bfloat16) for head in range(HA)], axis=0
        )
        keys = key_ref[pl.ds(base, WK), :]
        values = value_ref[pl.ds(base, WK), :]
        scores = (
            lax.dot_general(
                stacked, keys, (((1,), (1,)), ((), ())), preferred_element_type=jnp.float32
            )
            * scale
        )
        scores = scores + bias_ref[:, pl.ds(base, WQ), :].reshape(HA * WQ, WK).astype(jnp.float32)
        slot = first_ref[0] + base - RIM + lane
        inside = (slot >= bounds_ref[2 * index]) & (slot < bounds_ref[2 * index + 1])
        scores = jnp.where(inside, scores, FAR)
        weights = jnp.exp(scores - jnp.max(scores, axis=-1, keepdims=True))
        totals = jnp.sum(weights, axis=-1, keepdims=True)
        attended = matmul(weights.astype(jnp.bfloat16), values) / totals
        result = jnp.zeros((WQ, channels), jnp.float32)
        for head in range(HA):
            result = result + jnp.where(head_of == head, attended[head * WQ : (head + 1) * WQ], 0.0)
        held_ref[pl.ds(base, WQ), :] = result
        return carry

    lax.fori_loop(0, count // WQ, window, 0, unroll=UNROLL)
    gated = (held_ref[...] * jax.nn.sigmoid(gate_ref[...].astype(jnp.float32))).astype(jnp.bfloat16)
    fresh = state_ref[inner, :] + matmul(gated, weight_ref[6])
    final = layer_norm(fresh).astype(jnp.bfloat16)
    out_ref[...] = lax.dot_general(
        position_ref[...], final, (((1,), (1,)), ((), ())), preferred_element_type=jnp.float32
    )


UNROLL = 8


def atom_block(first, bounds, rows, skip, cond, owners, weights, vectors, positions, bias):
    count, channels = bias.shape[1], skip.shape[1]
    extended = skip.shape[0]
    smem = pl.BlockSpec(memory_space=pltpu.SMEM)
    vmem = pl.BlockSpec(memory_space=pltpu.VMEM)
    return pl.pallas_call(
        atom_kernel,
        in_specs=[smem, smem] + [vmem] * 8,
        out_specs=vmem,
        out_shape=jax.ShapeDtypeStruct((positions.shape[0], count), jnp.float32),
        scratch_shapes=[
            pltpu.VMEM((extended, channels), jnp.float32),
            pltpu.VMEM((count, channels), jnp.bfloat16),
            pltpu.VMEM((count, channels), jnp.bfloat16),
            pltpu.VMEM((extended, channels), jnp.bfloat16),
            pltpu.VMEM((extended, channels), jnp.bfloat16),
            pltpu.VMEM((count, channels), jnp.float32),
        ],
        compiler_params=pltpu.CompilerParams(vmem_limit_bytes=VMEM_LIMIT),
        name="atom_block",
    )(first, bounds, rows, skip, cond, owners, weights, vectors, positions, bias)


def rim_extended(array, axis):
    size, length = (lax.axis_size(axis), array.shape[0])
    up = [(i, (i + 1) % size) for i in range(size - 1)]
    down = [(j, i) for i, j in up]
    before = lax.ppermute(array[length - RIM :], axis, up)
    after = lax.ppermute(array[:RIM], axis, down)
    return jnp.concatenate([before, array, after], axis=0)


def per_device(
    token_act,
    token_cond,
    pair_bias,
    token_mask,
    ada_weights,
    attention_in,
    attention_out,
    transition_in,
    transition_out,
    token_vectors,
    atom_skip,
    atom_cond,
    atom_bias,
    window_bounds,
    atom_token,
    atom_weights,
    token_to_atom,
    atom_vectors,
    position_out,
):
    groups = lax.axis_size("fsdp")
    act_rows = token_act[0]
    row_count, depth = act_rows.shape
    column_count = attention_in.shape[2]
    channels = atom_cond.shape[1]
    start = lax.axis_index("fsdp") * column_count
    atom_pair = rim_extended(jnp.concatenate([atom_skip[0], atom_cond], axis=1), "seq")
    owners = rim_extended(atom_token, "seq")[:, None]

    cond_normed = layer_norm(token_cond[0]).astype(jnp.bfloat16)
    act_normed = layer_norm(act_rows).astype(jnp.bfloat16)
    act_slots = jnp.transpose(act_normed.reshape(row_count, groups, column_count), (1, 0, 2))
    cond_all, act_all, mask_all = move(
        1,
        (
            ("line", "fsdp", cond_normed),
            ("exchange", "fsdp", pack(act_slots)),
            ("paired", "seq", token_mask[None]),
        ),
    )
    cond_flat = cond_all.reshape(groups * row_count, depth)
    act_flat = unpack(act_all).reshape(groups * row_count, column_count).astype(jnp.float32)

    def adaptive(scale_index, shift_index, vector_index):
        offset = lax.dynamic_slice_in_dim(token_vectors[vector_index], start, column_count)
        scaled = jax.nn.sigmoid(matmul(cond_flat, ada_weights[scale_index]) + offset) * act_flat
        rows = (scaled + matmul(cond_flat, ada_weights[shift_index])).astype(jnp.bfloat16)
        return pack(rows.reshape(groups, row_count, column_count))

    def joined(array):
        array = unpack(array)
        return jnp.transpose(array, (1, 2, 0, 3)).reshape(groups * row_count, depth)

    (attend_all,) = move(2, (("line", "fsdp", adaptive(0, 1, 0)),))
    transit_part = adaptive(2, 3, 1)
    attend_flat = joined(attend_all)
    query_bias = lax.dynamic_slice_in_dim(token_vectors[2], start, column_count)

    def project(index):
        return matmul(attend_flat, attention_in[index])

    def grouped(array):
        return array.astype(jnp.bfloat16).reshape(groups, row_count, -1)

    keys_values = jnp.concatenate([grouped(project(1)), grouped(project(2))], axis=-1)
    kv_all, transit_all, small_all = move(
        3,
        (
            ("paired", "seq", keys_values),
            ("line", "fsdp", transit_part),
            (
                "line",
                "fsdp",
                jnp.concatenate(
                    [
                        atom_weights.reshape(-1, channels),
                        token_to_atom,
                    ],
                    axis=0,
                ),
            ),
        ),
    )
    query_rows = grouped(project(0) + query_bias)
    gate_rows = grouped(project(3))
    weight_rows = atom_weights.size // channels
    atom_full = jnp.transpose(
        small_all[:, :weight_rows].reshape((groups,) + atom_weights.shape), (1, 2, 0, 3)
    ).reshape(atom_weights.shape[0], channels, channels)
    project_full = small_all[:, weight_rows:].reshape(depth, channels)
    gated = token_attention(
        query_rows, gate_rows, kv_all, pair_bias, mask_all.reshape(1, -1)
    ).reshape(groups * row_count, -1)
    transit_flat = joined(transit_all)
    hidden = (
        jax.nn.silu(matmul(transit_flat, transition_in[0])) * matmul(transit_flat, transition_in[1])
    ).astype(jnp.bfloat16)
    partial_sum = matmul(gated, attention_out) + matmul(hidden, transition_out)
    (parts,) = move(
        4,
        (("exchange", "fsdp", partial_sum.astype(jnp.bfloat16).reshape(groups, row_count, depth)),),
    )
    combined = jnp.sum(parts.astype(jnp.float32), axis=0)
    token_result = (act_rows.astype(jnp.float32) + combined).astype(jnp.bfloat16)
    projected = matmul(token_result, project_full).astype(jnp.bfloat16)
    (all_rows,) = move(5, (("paired", "seq", projected),))
    first_atom = (lax.axis_index("seq") * atom_cond.shape[0]).astype(jnp.int32).reshape(1)
    update = atom_block(
        first_atom,
        window_bounds.reshape(-1),
        all_rows.reshape(-1, channels),
        atom_pair[:, :channels],
        atom_pair[:, channels:],
        owners,
        atom_full,
        atom_vectors,
        position_out,
        atom_bias,
    )
    return (token_result[None], update[None])


def solution(mesh):
    in_specs = (
        P(("sample", "fsdp"), "seq", None),
        P(("sample", "fsdp"), "seq", None),
        P("fsdp", "seq", None),
        P("seq"),
        P(None, None, "fsdp"),
        P(None, None, "fsdp"),
        P("fsdp", None),
        P(None, None, "fsdp"),
        P("fsdp", None),
        P(),
        P(("sample", "fsdp"), "seq", None),
        P("seq", None),
        P(None, "seq", None),
        P("seq", None),
        P("seq"),
        P(None, None, "fsdp"),
        P("fsdp", None),
        P(),
        P(),
    )
    out_specs = (P(("sample", "fsdp"), "seq", None), P(("sample", "fsdp"), None, "seq"))
    return jax.shard_map(
        per_device, mesh=mesh, in_specs=in_specs, out_specs=out_specs, check_vma=False
    )
```

```python
import functools
import math

import jax
import jax.numpy as jnp
from jax import lax
from jax.experimental import pallas as pl
from jax.experimental.pallas import tpu as pltpu
from jax.sharding import PartitionSpec as P

HA = 4
WQ = 32
WK = 128
HD = 48
EPS = 1e-05
FAR = -1e30
RIM = (WK - WQ) // 2
VMEM_LIMIT = 56 * 1024 * 1024
MESH = pl.DeviceIdType.MESH


def layer_norm(values):
    values = values.astype(jnp.float32)
    center = values - jnp.mean(values, axis=-1, keepdims=True)
    spread = jnp.mean(center * center, axis=-1, keepdims=True)
    return center * lax.rsqrt(spread + EPS)


def matmul(left_side, right_side):
    return jnp.dot(left_side, right_side, preferred_element_type=jnp.float32)


def pack(array):
    half = array.shape[-2] // 2
    return jnp.concatenate([array[..., :half, :], array[..., half:, :]], axis=-1)


def unpack(array):
    half = array.shape[-1] // 2
    return jnp.concatenate([array[..., :half], array[..., half:]], axis=-2)


class Line:
    def __init__(self, axis, size, paired, block, out, send, recv, local, partner_send, partner_recv):
        self.axis, self.size, self.paired = axis, size, paired
        self.block, self.out, self.send, self.recv, self.local = block, out, send, recv, local
        self.partner_send, self.partner_recv = partner_send, partner_recv
        self.index = lax.axis_index(axis)
        self.stride = 2 if paired else 1
        self.length = size // self.stride
        self.position = self.index // 2 if paired else self.index
        self.parity = self.index - 2 * self.position if paired else 0

    def slot(self, position):
        return position * self.stride + self.parity

    def partner(self):
        return self.index + 1 - 2 * self.parity

    def guards(self, side, step):
        here, last = self.position, self.length - 1
        if side == 0:
            return (here - step >= 0) & (here < last), here - 1 - step >= 0
        return (here + step <= last) & (here > 0), here + 1 + step <= last

    def copy(self, side, step, arriving):
        sign = 1 if side == 0 else -1
        origin = self.position - sign * (step + (1 if arriving else 0))
        target = self.slot(self.position + sign)
        slot = self.slot(origin)
        source = self.block if (step == 0 and not arriving) else self.out.at[slot]
        return pltpu.make_async_remote_copy(
            src_ref=source,
            dst_ref=self.out.at[slot],
            send_sem=self.send.at[side, step],
            recv_sem=self.recv.at[side, step],
            device_id={self.axis: target},
            device_id_type=MESH,
        )

    def hand(self, key, origin, own, arriving):
        slot = self.slot(origin)
        landing = origin * 2 + 1 - self.parity if arriving else slot
        return pltpu.make_async_remote_copy(
            src_ref=self.block if own else self.out.at[slot],
            dst_ref=self.out.at[landing],
            send_sem=self.partner_send.at[key],
            recv_sem=self.partner_recv.at[key],
            device_id={self.axis: self.partner()},
            device_id_type=MESH,
        )

    def greet(self, barrier):
        def neighbour(target):
            pl.semaphore_signal(barrier, inc=1, device_id={self.axis: target}, device_id_type=MESH)

        expected = 0
        if self.length > 1:
            above = self.position > 0
            below = self.position < self.length - 1

            @pl.when(above)
            def _():
                neighbour(self.slot(self.position - 1))

            @pl.when(below)
            def _():
                neighbour(self.slot(self.position + 1))

            expected = jnp.where(above, 1, 0) + jnp.where(below, 1, 0)
        if self.paired:
            neighbour(self.partner())
            expected = expected + 1
        return expected

    def begin(self):
        pltpu.make_async_copy(self.block, self.out.at[self.index], self.local.at[0]).start()
        if self.paired:
            self.hand(0, self.position, True, False).start()

    def advance(self, step):
        for side in (0, 1):
            goes, unused = self.guards(side, step)
            if step > 0:
                self.arrive(side, step - 1)

            @pl.when(goes)
            def _():
                self.copy(side, step, False).start()

    def arrive(self, side, step):
        unused, comes = self.guards(side, step)

        @pl.when(comes)
        def _():
            self.copy(side, step, True).wait_recv()
            if self.paired:
                origin = self.position - (step + 1) if side == 0 else self.position + step + 1
                self.hand(1 + side * (self.length - 1) + step, origin, False, False).start()

    def steps(self):
        return self.length - 1

    def finish(self):
        last = self.length - 1
        if last > 0:
            for side in (0, 1):
                self.arrive(side, last - 1)
        for side in (0, 1):
            for step in range(last):
                goes, comes = self.guards(side, step)

                @pl.when(goes)
                def _():
                    self.copy(side, step, False).wait_send()

                if self.paired:

                    @pl.when(comes)
                    def _():
                        origin = self.position - (step + 1) if side == 0 else self.position + step + 1
                        key = 1 + side * last + step
                        self.hand(key, origin, False, False).wait_send()
                        self.hand(key, origin, False, True).wait_recv()

        if self.paired:
            self.hand(0, self.position, True, False).wait_send()
            self.hand(0, self.position, True, True).wait_recv()
        pltpu.make_async_copy(self.block, self.out.at[self.index], self.local.at[0]).wait()


class Exchange:
    def __init__(self, axis, size, block, out, send, recv, local):
        self.axis, self.size, self.block, self.out = axis, size, block, out
        self.send, self.recv, self.local = send, recv, local
        self.index = lax.axis_index(axis)

    def peer(self, shift):
        return lax.rem(self.index + shift, self.size)

    def greet(self, barrier):
        for shift in range(1, self.size):
            pl.semaphore_signal(
                barrier, inc=1, device_id={self.axis: self.peer(shift)}, device_id_type=MESH
            )
        return self.size - 1

    def copy(self, shift, arriving):
        landing = self.peer(self.size - shift) if arriving else self.index
        return pltpu.make_async_remote_copy(
            src_ref=self.block.at[self.peer(shift)],
            dst_ref=self.out.at[landing],
            send_sem=self.send.at[shift],
            recv_sem=self.recv.at[shift],
            device_id={self.axis: self.peer(shift)},
            device_id_type=MESH,
        )

    def begin(self):
        pltpu.make_async_copy(
            self.block.at[self.index], self.out.at[self.index], self.local.at[0]
        ).start()
        for shift in range(1, self.size):
            self.copy(shift, False).start()

    def steps(self):
        return 0

    def advance(self, step):
        pass

    def finish(self):
        for shift in range(1, self.size):
            self.copy(shift, False).wait_send()
            self.copy(shift, True).wait_recv()
        pltpu.make_async_copy(
            self.block.at[self.index], self.out.at[self.index], self.local.at[0]
        ).wait()


class Halo:
    def __init__(self, axis, size, block, out, send, recv):
        self.axis, self.size, self.block, self.out = axis, size, block, out
        self.send, self.recv = send, recv
        self.index = lax.axis_index(axis)
        self.above, self.below = self.index > 0, self.index < size - 1

    def greet(self, barrier):
        for present, target in ((self.above, self.index - 1), (self.below, self.index + 1)):

            @pl.when(present)
            def _():
                pl.semaphore_signal(
                    barrier, inc=1, device_id={self.axis: target}, device_id_type=MESH
                )

        return jnp.where(self.above, 1, 0) + jnp.where(self.below, 1, 0)

    def copy(self, side):
        return pltpu.make_async_remote_copy(
            src_ref=self.block.at[side],
            dst_ref=self.out.at[1 - side],
            send_sem=self.send.at[side],
            recv_sem=self.recv.at[side],
            device_id={self.axis: self.index - 1 + 2 * side},
            device_id_type=MESH,
        )

    def begin(self):
        for side, present in ((0, self.above), (1, self.below)):

            @pl.when(present)
            def _():
                self.copy(side).start()

            @pl.when(jnp.logical_not(present))
            def _():
                self.out[side] = jnp.zeros(self.out.shape[1:], self.out.dtype)

    def steps(self):
        return 0

    def finish(self):
        for side, present in ((0, self.above), (1, self.below)):

            @pl.when(present)
            def _():
                self.copy(side).wait_send()
                self.copy(1 - side).wait_recv()


class Swap:
    def __init__(self, axis, size, block, out, send, recv, local):
        self.axis, self.block, self.out = axis, block, out
        self.send, self.recv, self.local = send, recv, local
        self.index = lax.axis_index(axis)
        self.parity = lax.rem(self.index, 2)

    def copy(self, arriving):
        return pltpu.make_async_remote_copy(
            src_ref=self.block,
            dst_ref=self.out.at[1 - self.parity if arriving else self.parity],
            send_sem=self.send.at[0],
            recv_sem=self.recv.at[0],
            device_id={self.axis: self.index + 1 - 2 * self.parity},
            device_id_type=MESH,
        )

    def begin(self):
        pltpu.make_async_copy(self.block, self.out.at[self.parity], self.local.at[0]).start()
        self.copy(False).start()

    def steps(self):
        return 0

    def finish(self):
        self.copy(False).wait_send()
        self.copy(True).wait_recv()
        pltpu.make_async_copy(self.block, self.out.at[self.parity], self.local.at[0]).wait()


def line_scratch(size, paired):
    dma = pltpu.SemaphoreType.DMA
    length = size // 2 if paired else size
    steps = max(length - 1, 1)
    scratch = [dma((2, steps)), dma((2, steps)), dma((1,))]
    if paired:
        scratch += [dma((2 * length,)), dma((2 * length,))]
    return scratch


def run_flows(flows):
    for flow in flows:
        flow.begin()
    for step in range(max(flow.steps() for flow in flows)):
        for flow in flows:
            if step < flow.steps():
                flow.advance(step)
    for flow in flows:
        flow.finish()


def move_kernel(kinds, *refs):
    count = len(kinds)
    blocks, outs, sems = refs[:count], refs[count : 2 * count], list(refs[2 * count :])
    flows, leaders = [], {}

    def take(number):
        taken = sems[:number]
        del sems[:number]
        return taken

    for (kind, axis, size, chunks), block, out in zip(kinds, blocks, outs):
        if kind == "exchange":
            flow = Exchange(axis, size, block, out, *take(3))
            leaders[axis] = flow
            flows.append(flow)
        elif kind == "halo":
            flows.append(Halo(axis, size, block, out, *take(2)))
        elif kind == "swap":
            flows.append(Swap(axis, size, block, out, *take(3)))
        else:
            paired = kind == "paired"
            rows = block.shape[0] // chunks
            for chunk in range(chunks):
                part = pl.ds(chunk * rows, rows)
                flow = Line(
                    axis, size, paired, block.at[part], ChunkedOut(out, part),
                    *take(5 if paired else 3), *(() if paired else (None, None)),
                )
                flows.append(flow)
        leaders.setdefault(axis, flows[-1])
    barrier = pltpu.get_barrier_semaphore()
    expected = 0
    for flow in leaders.values():
        expected = expected + flow.greet(barrier)
    pl.semaphore_wait(barrier, expected)
    run_flows(flows)


class ChunkedOut:
    def __init__(self, out, part):
        self.out, self.part = out, part

    @property
    def at(self):
        return self

    def __getitem__(self, slot):
        return self.out.at[slot, self.part]


def move(identity, items):
    kinds, arrays, shapes, scratch = [], [], [], []
    sent = 0
    for kind, axis, array, chunks in items:
        size = lax.axis_size(axis)
        kinds.append((kind, axis, size, chunks))
        arrays.append(array)
        lead = {"exchange": (), "halo": (), "swap": (2,)}.get(kind, (size,))
        shapes.append(jax.ShapeDtypeStruct(lead + array.shape, array.dtype))
        sent += array.size * array.dtype.itemsize
        dma = pltpu.SemaphoreType.DMA
        if kind == "exchange":
            scratch += [dma((size,)), dma((size,)), dma((1,))]
        elif kind == "halo":
            scratch += [dma((2,)), dma((2,))]
        elif kind == "swap":
            scratch += [dma((1,)), dma((1,)), dma((1,))]
        else:
            scratch += line_scratch(size, kind == "paired") * chunks
    return pl.pallas_call(
        functools.partial(move_kernel, tuple(kinds)),
        out_shape=tuple(shapes),
        in_specs=[pl.BlockSpec(memory_space=pltpu.VMEM)] * len(arrays),
        out_specs=tuple([pl.BlockSpec(memory_space=pltpu.VMEM)] * len(arrays)),
        scratch_shapes=scratch,
        compiler_params=pltpu.CompilerParams(
            collective_id=identity, has_side_effects=True, vmem_limit_bytes=VMEM_LIMIT
        ),
        cost_estimate=pl.CostEstimate(flops=0, bytes_accessed=30 * sent, transcendentals=0),
        name=f"move{identity}",
    )(*arrays)


def close_kernel(
    axis, size, row_axis, row_size, chunks, part_ref, act_ref, project_ref, token_ref, rows_ref,
    came_ref, sum_ref, total_ref, block_ref, send, recv, *line_sems,
):
    position = lax.axis_index(axis)
    above, below = position > 0, position < size - 1
    line = Line(row_axis, row_size, True, block_ref, rows_ref, *line_sems)
    barrier = pltpu.get_barrier_semaphore()
    expected = line.greet(barrier) + jnp.where(above, 1, 0) + jnp.where(below, 1, 0)
    for present, target in ((above, position - 1), (below, position + 1)):

        @pl.when(present)
        def _():
            pl.semaphore_signal(barrier, inc=1, device_id={axis: target}, device_id_type=MESH)

    pl.semaphore_wait(barrier, expected)
    height = part_ref.shape[1] // chunks
    sides = ((above, 1), (below, -1))

    def hop(side, step, chunk, relayed):
        goal = size - 1 - step if side == 0 else step
        rows = pl.ds(chunk * height, height)
        source = sum_ref.at[side, goal, rows] if relayed else part_ref.at[goal, rows]
        return pltpu.make_async_remote_copy(
            src_ref=source,
            dst_ref=came_ref.at[side, goal, rows],
            send_sem=send.at[side, step, chunk],
            recv_sem=recv.at[side, step, chunk],
            device_id={axis: position + sides[side][1]},
            device_id_type=MESH,
        )

    def each(action):
        for step in range(size - 1):
            goal_right, goal_left = size - 1 - step, step
            for chunk in range(chunks):
                for side in (0, 1):
                    goal = goal_right if side == 0 else goal_left
                    goes = position < goal if side == 0 else position > goal
                    action(side, step, chunk, goal, goes, sides[side][0])

    def forward(side, step, chunk, goal, goes, fed):
        rows = pl.ds(chunk * height, height)

        @pl.when(goes & fed)
        def _():
            hop(side, step, chunk, True).wait_recv()
            sum_ref[side, goal, rows] = (
                came_ref[side, goal, rows].astype(jnp.float32)
                + part_ref[goal, rows].astype(jnp.float32)
            ).astype(jnp.bfloat16)
            hop(side, step, chunk, True).start()

        @pl.when(goes & jnp.logical_not(fed))
        def _():
            hop(side, step, chunk, False).start()

    each(forward)
    total_ref[...] = act_ref[...].astype(jnp.float32) + part_ref[position].astype(jnp.float32)

    def collect(side, step, chunk, goal, goes, fed):
        rows = pl.ds(chunk * height, height)

        @pl.when((position == goal) & fed)
        def _():
            hop(side, step, chunk, True).wait_recv()
            total_ref[rows] = total_ref[rows] + came_ref[side, goal, rows].astype(jnp.float32)

    each(collect)
    token = total_ref[...].astype(jnp.bfloat16)
    token_ref[...] = token
    block_ref[...] = matmul(token, project_ref[...]).astype(jnp.bfloat16)
    run_flows([line])

    def settle(side, step, chunk, goal, goes, fed):
        @pl.when(goes)
        def _():
            hop(side, step, chunk, True).wait_send()

    each(settle)


def close(identity, axis, row_axis, parts, act_rows, project):
    size, row_size, chunks = lax.axis_size(axis), lax.axis_size(row_axis), 2
    rows, depth = act_rows.shape
    dma = pltpu.SemaphoreType.DMA
    vmem = pl.BlockSpec(memory_space=pltpu.VMEM)
    return pl.pallas_call(
        functools.partial(close_kernel, axis, size, row_axis, row_size, chunks),
        out_shape=(
            jax.ShapeDtypeStruct((rows, depth), jnp.bfloat16),
            jax.ShapeDtypeStruct((row_size, rows, project.shape[1]), jnp.bfloat16),
        ),
        in_specs=[vmem] * 3,
        out_specs=(vmem, vmem),
        scratch_shapes=[
            pltpu.VMEM((2,) + parts.shape, jnp.bfloat16),
            pltpu.VMEM((2,) + parts.shape, jnp.bfloat16),
            pltpu.VMEM((rows, depth), jnp.float32),
            pltpu.VMEM((rows, project.shape[1]), jnp.bfloat16),
            dma((2, size - 1, chunks)),
            dma((2, size - 1, chunks)),
        ]
        + line_scratch(row_size, True),
        compiler_params=pltpu.CompilerParams(
            collective_id=identity, has_side_effects=True, vmem_limit_bytes=VMEM_LIMIT
        ),
        name="close",
    )(parts, act_rows, project)


def attention_kernel(heads, span, q_ref, gate_ref, kv_ref, bias_ref, mask_ref, out_ref):
    rows, width = q_ref.shape[1], q_ref.shape[2]
    pieces, piece_rows = kv_ref.shape[0], kv_ref.shape[2]
    queries = q_ref[0]
    head_of = lax.broadcasted_iota(jnp.int32, (rows, width), 1) // HD
    stacked = jnp.concatenate(
        [jnp.where(head_of == head, queries, 0).astype(jnp.bfloat16) for head in range(heads)], axis=0
    )
    scale = 1.0 / math.sqrt(HD)
    maxima = totals = summed = None
    for first in range(0, pieces, span):
        taken = min(span, pieces - first)
        keys = jnp.concatenate([kv_ref[first + i, 0, :, :width] for i in range(taken)], axis=0)
        values = jnp.concatenate([kv_ref[first + i, 0, :, width:] for i in range(taken)], axis=0)
        columns = pl.ds(first * piece_rows, taken * piece_rows)
        scores = (
            lax.dot_general(
                stacked, keys, (((1,), (1,)), ((), ())), preferred_element_type=jnp.float32
            )
            * scale
        )
        bias = bias_ref[:, :, columns].reshape(heads * rows, taken * piece_rows)
        scores = scores + bias.astype(jnp.float32)
        scores = jnp.where(mask_ref[:, columns] > 0, scores, FAR)
        block_max = jnp.max(scores, axis=-1, keepdims=True)
        new_maxima = block_max if maxima is None else jnp.maximum(maxima, block_max)
        weights = jnp.exp(scores - new_maxima)
        block_total = jnp.sum(weights, axis=-1, keepdims=True)
        update = matmul(weights.astype(jnp.bfloat16), values)
        if maxima is None:
            totals, summed = block_total, update
        else:
            factor = jnp.exp(maxima - new_maxima)
            totals = totals * factor + block_total
            summed = summed * factor + update
        maxima = new_maxima
    attended = summed / totals
    result = jnp.zeros((rows, width), jnp.float32)
    for head in range(heads):
        result = result + jnp.where(head_of == head, attended[head * rows : (head + 1) * rows], 0.0)
    gate = jax.nn.sigmoid(gate_ref[0].astype(jnp.float32))
    out_ref[0] = (result * gate).astype(jnp.bfloat16)


def token_attention(query_rows, gate_rows, kv_all, pair_bias, mask_row):
    groups, rows, width = query_rows.shape
    heads, keys = pair_bias.shape[0], pair_bias.shape[2]
    pieces, piece_rows = kv_all.shape[0], kv_all.shape[2]
    one = lambda g: (g, 0, 0)
    return pl.pallas_call(
        functools.partial(attention_kernel, heads, max(512 // piece_rows, 1)),
        grid=(groups,),
        in_specs=[
            pl.BlockSpec((1, rows, width), one),
            pl.BlockSpec((1, rows, width), one),
            pl.BlockSpec((pieces, 1, piece_rows, 2 * width), lambda g: (0, g, 0, 0)),
            pl.BlockSpec((heads, rows, keys), lambda g: (0, 0, 0)),
            pl.BlockSpec((1, keys), lambda g: (0, 0)),
        ],
        out_specs=pl.BlockSpec((1, rows, width), one),
        out_shape=jax.ShapeDtypeStruct((groups, rows, width), jnp.bfloat16),
        compiler_params=pltpu.CompilerParams(vmem_limit_bytes=VMEM_LIMIT),
        name="token_attention",
    )(query_rows, gate_rows, kv_all, pair_bias, mask_row)


def atom_kernel(
    first_ref, bounds_ref, rows_ref, skip_ref, cond_ref, rim_ref, token_ref, weight_ref, vector_ref,
    position_ref, bias_ref, out_ref, state_ref, query_ref, gate_ref, key_ref, value_ref, held_ref,
):
    count, channels = query_ref.shape
    head_width = channels // HA
    tokens = rows_ref.shape[0]
    chunk = min(512, tokens)
    inner = pl.ds(RIM, count)
    owners = token_ref[...]
    taken = jnp.zeros((owners.shape[0], channels), jnp.float32)
    for start in range(0, tokens, chunk):
        column = lax.broadcasted_iota(jnp.int32, (owners.shape[0], chunk), 1) + start
        hit = jnp.where(owners == column, 1.0, 0.0).astype(jnp.bfloat16)
        taken = taken + matmul(hit, rows_ref[start : start + chunk, :])
    skip = jnp.concatenate([rim_ref[0, :, :channels], skip_ref[...], rim_ref[1, :, :channels]], axis=0)
    cond = jnp.concatenate([rim_ref[0, :, channels:], cond_ref[...], rim_ref[1, :, channels:]], axis=0)
    state = skip.astype(jnp.float32) + taken
    state_ref[...] = state
    normed = layer_norm(cond).astype(jnp.bfloat16)
    atom_x = (
        jax.nn.sigmoid(matmul(normed, weight_ref[0]) + vector_ref[0:1, :]) * layer_norm(state)
        + matmul(normed, weight_ref[1])
    ).astype(jnp.bfloat16)
    own_x = atom_x[RIM : RIM + count, :]
    query_ref[...] = (matmul(own_x, weight_ref[2]) + vector_ref[1:2, :]).astype(jnp.bfloat16)
    gate_ref[...] = matmul(own_x, weight_ref[5]).astype(jnp.bfloat16)
    key_ref[...] = matmul(atom_x, weight_ref[3]).astype(jnp.bfloat16)
    value_ref[...] = matmul(atom_x, weight_ref[4]).astype(jnp.bfloat16)
    head_of = lax.broadcasted_iota(jnp.int32, (WQ, channels), 1) // head_width
    lane = lax.broadcasted_iota(jnp.int32, (1, WK), 1)
    scale = 1.0 / math.sqrt(head_width)

    def windows(step, carry):
        scores = []
        bases = [pl.multiple_of(step * (BATCH * WQ) + i * WQ, WQ) for i in range(BATCH)]
        for i, base in enumerate(bases):
            queries = query_ref[pl.ds(base, WQ), :]
            stacked = jnp.concatenate(
                [jnp.where(head_of == head, queries, 0).astype(jnp.bfloat16) for head in range(HA)],
                axis=0,
            )
            score = lax.dot_general(
                stacked, key_ref[pl.ds(base, WK), :], (((1,), (1,)), ((), ())),
                preferred_element_type=jnp.float32,
            )
            bias = bias_ref[:, pl.ds(base, WQ), :].reshape(HA * WQ, WK).astype(jnp.float32)
            slot = first_ref[0] + base - RIM + lane
            index = step * BATCH + i
            inside = (slot >= bounds_ref[2 * index]) & (slot < bounds_ref[2 * index + 1])
            scores.append(jnp.where(inside, score * scale + bias, FAR))
        weights = [jnp.exp(score - jnp.max(score, axis=-1, keepdims=True)) for score in scores]
        results = []
        for base, weight in zip(bases, weights):
            attended = matmul(weight.astype(jnp.bfloat16), value_ref[pl.ds(base, WK), :])
            attended = attended / jnp.sum(weight, axis=-1, keepdims=True)
            result = jnp.zeros((WQ, channels), jnp.float32)
            for head in range(HA):
                result = result + jnp.where(
                    head_of == head, attended[head * WQ : (head + 1) * WQ], 0.0
                )
            results.append(result)
        start = pl.multiple_of(step * (BATCH * WQ), BATCH * WQ)
        held_ref[pl.ds(start, BATCH * WQ), :] = jnp.concatenate(results, axis=0)
        return carry

    lax.fori_loop(0, count // (BATCH * WQ), windows, 0)
    gated = (held_ref[...] * jax.nn.sigmoid(gate_ref[...].astype(jnp.float32))).astype(jnp.bfloat16)
    fresh = state_ref[inner, :] + matmul(gated, weight_ref[6])
    final = layer_norm(fresh).astype(jnp.bfloat16)
    out_ref[...] = lax.dot_general(
        position_ref[...], final, (((1,), (1,)), ((), ())), preferred_element_type=jnp.float32
    )


BATCH = 8


def atom_block(first, bounds, rows, skip, cond, rims, owners, weights, vectors, positions, bias):
    count, channels = bias.shape[1], skip.shape[1]
    extended = skip.shape[0] + 2 * RIM
    smem = pl.BlockSpec(memory_space=pltpu.SMEM)
    vmem = pl.BlockSpec(memory_space=pltpu.VMEM)
    return pl.pallas_call(
        atom_kernel,
        in_specs=[smem, smem] + [vmem] * 9,
        out_specs=vmem,
        out_shape=jax.ShapeDtypeStruct((positions.shape[0], count), jnp.float32),
        scratch_shapes=[
            pltpu.VMEM((extended, channels), jnp.float32),
            pltpu.VMEM((count, channels), jnp.bfloat16),
            pltpu.VMEM((count, channels), jnp.bfloat16),
            pltpu.VMEM((extended, channels), jnp.bfloat16),
            pltpu.VMEM((extended, channels), jnp.bfloat16),
            pltpu.VMEM((count, channels), jnp.float32),
        ],
        compiler_params=pltpu.CompilerParams(vmem_limit_bytes=VMEM_LIMIT),
        name="atom_block",
    )(first, bounds, rows, skip, cond, rims, owners, weights, vectors, positions, bias)


def rims(array):
    return jnp.stack([array[:RIM], array[array.shape[0] - RIM :]])


def per_device(
    token_act,
    token_cond,
    pair_bias,
    token_mask,
    ada_weights,
    attention_in,
    attention_out,
    transition_in,
    transition_out,
    token_vectors,
    atom_skip,
    atom_cond,
    atom_bias,
    window_bounds,
    atom_token,
    atom_weights,
    token_to_atom,
    atom_vectors,
    position_out,
):
    groups = lax.axis_size("fsdp")
    act_rows = token_act[0]
    row_count, depth = act_rows.shape
    column_count = attention_in.shape[2]
    channels = atom_cond.shape[1]
    start = lax.axis_index("fsdp") * column_count
    atom_rims = rims(jnp.concatenate([atom_skip[0], atom_cond], axis=1))
    owner_rims = jnp.pad(rims(atom_token)[:, None, :], ((0, 0), (0, 0), (0, 2 * WK - RIM)))
    small = jnp.concatenate([atom_weights.reshape(-1, channels), token_to_atom], axis=0)
    small_height = small.shape[0] // 2
    small_half = lax.dynamic_slice_in_dim(
        small, lax.rem(lax.axis_index("seq"), 2) * small_height, small_height
    )

    cond_normed = layer_norm(token_cond[0]).astype(jnp.bfloat16)
    act_normed = layer_norm(act_rows).astype(jnp.bfloat16)
    act_slots = jnp.transpose(act_normed.reshape(row_count, groups, column_count), (1, 0, 2))
    cond_all, act_all, atom_rims, owner_rims = move(
        1,
        (
            ("line", "fsdp", cond_normed, 4),
            ("exchange", "fsdp", pack(act_slots), 1),
            ("halo", "seq", atom_rims, 1),
            ("halo", "seq", owner_rims, 1),
        ),
    )
    owners = jnp.concatenate([owner_rims[0, 0, :RIM], atom_token, owner_rims[1, 0, :RIM]])[:, None]
    cond_flat = cond_all.reshape(groups * row_count, depth)
    act_flat = unpack(act_all).reshape(groups * row_count, column_count).astype(jnp.float32)

    def adaptive(scale_index, shift_index, vector_index):
        offset = lax.dynamic_slice_in_dim(token_vectors[vector_index], start, column_count)
        scaled = jax.nn.sigmoid(matmul(cond_flat, ada_weights[scale_index]) + offset) * act_flat
        rows = (scaled + matmul(cond_flat, ada_weights[shift_index])).astype(jnp.bfloat16)
        return pack(rows.reshape(groups, row_count, column_count))

    def joined(array):
        array = unpack(array)
        return jnp.transpose(array, (1, 2, 0, 3)).reshape(groups * row_count, depth)

    attend_all, small_halves = move(
        2, (("line", "fsdp", adaptive(0, 1, 0), groups), ("line", "fsdp", small_half, 1))
    )
    transit_part = adaptive(2, 3, 1)
    attend_flat = joined(attend_all)
    query_bias = lax.dynamic_slice_in_dim(token_vectors[2], start, column_count)

    def project(index):
        return matmul(attend_flat, attention_in[index])

    def grouped(array):
        return array.astype(jnp.bfloat16).reshape(groups, row_count, -1)

    keys_values = jnp.concatenate([grouped(project(1)), grouped(project(2))], axis=-1)
    kv_all, transit_all, mask_all, small_all = move(
        3,
        (
            ("paired", "seq", keys_values, groups),
            ("line", "fsdp", transit_part, groups),
            ("paired", "seq", token_mask[None], 1),
            ("swap", "seq", small_halves, 1),
        ),
    )
    small_all = jnp.transpose(small_all, (1, 0, 2, 3)).reshape(groups, -1, channels)
    query_rows = grouped(project(0) + query_bias)
    gate_rows = grouped(project(3))
    weight_rows = atom_weights.size // channels
    atom_full = jnp.transpose(
        small_all[:, :weight_rows].reshape((groups,) + atom_weights.shape), (1, 2, 0, 3)
    ).reshape(atom_weights.shape[0], channels, channels)
    project_full = small_all[:, weight_rows:].reshape(depth, channels)
    gated = token_attention(
        query_rows, gate_rows, kv_all, pair_bias, mask_all.reshape(1, -1)
    ).reshape(groups * row_count, -1)
    transit_flat = joined(transit_all)
    hidden = (
        jax.nn.silu(matmul(transit_flat, transition_in[0])) * matmul(transit_flat, transition_in[1])
    ).astype(jnp.bfloat16)
    partial_sum = matmul(gated, attention_out) + matmul(hidden, transition_out)
    token_result, all_rows = close(
        4,
        "fsdp",
        "seq",
        partial_sum.astype(jnp.bfloat16).reshape(groups, row_count, depth),
        act_rows,
        project_full,
    )
    first_atom = (lax.axis_index("seq") * atom_cond.shape[0]).astype(jnp.int32).reshape(1)
    update = atom_block(
        first_atom,
        window_bounds.reshape(-1),
        all_rows.reshape(-1, channels),
        atom_skip[0],
        atom_cond,
        atom_rims,
        owners,
        atom_full,
        atom_vectors,
        position_out,
        atom_bias,
    )
    return (token_result[None], update[None])


def solution(mesh):
    in_specs = (
        P(("sample", "fsdp"), "seq", None),
        P(("sample", "fsdp"), "seq", None),
        P("fsdp", "seq", None),
        P("seq"),
        P(None, None, "fsdp"),
        P(None, None, "fsdp"),
        P("fsdp", None),
        P(None, None, "fsdp"),
        P("fsdp", None),
        P(),
        P(("sample", "fsdp"), "seq", None),
        P("seq", None),
        P(None, "seq", None),
        P("seq", None),
        P("seq"),
        P(None, None, "fsdp"),
        P("fsdp", None),
        P(),
        P(),
    )
    out_specs = (P(("sample", "fsdp"), "seq", None), P(("sample", "fsdp"), None, "seq"))
    return jax.shard_map(
        per_device, mesh=mesh, in_specs=in_specs, out_specs=out_specs, check_vma=False
    )
```

```python
import functools
import math

import jax
import jax.numpy as jnp
from jax import lax
from jax.experimental import pallas as pl
from jax.experimental.pallas import tpu as pltpu
from jax.sharding import PartitionSpec as P

HA = 4
WQ = 32
WK = 128
HD = 48
EPS = 1e-05
FAR = -1e30
RIM = (WK - WQ) // 2
VMEM_LIMIT = 56 * 1024 * 1024
MESH = pl.DeviceIdType.MESH


def layer_norm(values):
    values = values.astype(jnp.float32)
    center = values - jnp.mean(values, axis=-1, keepdims=True)
    spread = jnp.mean(center * center, axis=-1, keepdims=True)
    return center * lax.rsqrt(spread + EPS)


def matmul(left_side, right_side):
    return jnp.dot(left_side, right_side, preferred_element_type=jnp.float32)


def pack(array):
    half = array.shape[-2] // 2
    return jnp.concatenate([array[..., :half, :], array[..., half:, :]], axis=-1)


def unpack(array):
    half = array.shape[-1] // 2
    return jnp.concatenate([array[..., :half], array[..., half:]], axis=-2)


class Line:
    def __init__(self, axis, size, paired, block, out, send, recv, local, partner_send, partner_recv):
        self.axis, self.size, self.paired = axis, size, paired
        self.block, self.out, self.send, self.recv, self.local = block, out, send, recv, local
        self.partner_send, self.partner_recv = partner_send, partner_recv
        self.index = lax.axis_index(axis)
        self.stride = 2 if paired else 1
        self.length = size // self.stride
        self.position = self.index // 2 if paired else self.index
        self.parity = self.index - 2 * self.position if paired else 0

    def slot(self, position):
        return position * self.stride + self.parity

    def partner(self):
        return self.index + 1 - 2 * self.parity

    def guards(self, side, step):
        here, last = self.position, self.length - 1
        if side == 0:
            return (here - step >= 0) & (here < last), here - 1 - step >= 0
        return (here + step <= last) & (here > 0), here + 1 + step <= last

    def copy(self, side, step, arriving):
        sign = 1 if side == 0 else -1
        origin = self.position - sign * (step + (1 if arriving else 0))
        target = self.slot(self.position + sign)
        slot = self.slot(origin)
        source = self.block if (step == 0 and not arriving) else self.out.at[slot]
        return pltpu.make_async_remote_copy(
            src_ref=source,
            dst_ref=self.out.at[slot],
            send_sem=self.send.at[side, step],
            recv_sem=self.recv.at[side, step],
            device_id={self.axis: target},
            device_id_type=MESH,
        )

    def hand(self, key, origin, own, arriving):
        slot = self.slot(origin)
        landing = origin * 2 + 1 - self.parity if arriving else slot
        return pltpu.make_async_remote_copy(
            src_ref=self.block if own else self.out.at[slot],
            dst_ref=self.out.at[landing],
            send_sem=self.partner_send.at[key],
            recv_sem=self.partner_recv.at[key],
            device_id={self.axis: self.partner()},
            device_id_type=MESH,
        )

    def greet(self, barrier):
        def neighbour(target):
            pl.semaphore_signal(barrier, inc=1, device_id={self.axis: target}, device_id_type=MESH)

        expected = 0
        if self.length > 1:
            above = self.position > 0
            below = self.position < self.length - 1

            @pl.when(above)
            def _():
                neighbour(self.slot(self.position - 1))

            @pl.when(below)
            def _():
                neighbour(self.slot(self.position + 1))

            expected = jnp.where(above, 1, 0) + jnp.where(below, 1, 0)
        if self.paired:
            neighbour(self.partner())
            expected = expected + 1
        return expected

    def begin(self):
        pltpu.make_async_copy(self.block, self.out.at[self.index], self.local.at[0]).start()
        if self.paired:
            self.hand(0, self.position, True, False).start()

    def advance(self, step):
        for side in (0, 1):
            goes, unused = self.guards(side, step)
            if step > 0:
                self.arrive(side, step - 1)

            @pl.when(goes)
            def _():
                self.copy(side, step, False).start()

    def arrive(self, side, step):
        unused, comes = self.guards(side, step)

        @pl.when(comes)
        def _():
            self.copy(side, step, True).wait_recv()
            if self.paired:
                origin = self.position - (step + 1) if side == 0 else self.position + step + 1
                self.hand(1 + side * (self.length - 1) + step, origin, False, False).start()

    def steps(self):
        return self.length - 1

    def finish(self):
        last = self.length - 1
        if last > 0:
            for side in (0, 1):
                self.arrive(side, last - 1)
        for side in (0, 1):
            for step in range(last):
                goes, comes = self.guards(side, step)

                @pl.when(goes)
                def _():
                    self.copy(side, step, False).wait_send()

                if self.paired:

                    @pl.when(comes)
                    def _():
                        origin = self.position - (step + 1) if side == 0 else self.position + step + 1
                        key = 1 + side * last + step
                        self.hand(key, origin, False, False).wait_send()
                        self.hand(key, origin, False, True).wait_recv()

        if self.paired:
            self.hand(0, self.position, True, False).wait_send()
            self.hand(0, self.position, True, True).wait_recv()
        pltpu.make_async_copy(self.block, self.out.at[self.index], self.local.at[0]).wait()


class Exchange:
    def __init__(self, axis, size, block, out, send, recv, local):
        self.axis, self.size, self.block, self.out = axis, size, block, out
        self.send, self.recv, self.local = send, recv, local
        self.index = lax.axis_index(axis)

    def peer(self, shift):
        return lax.rem(self.index + shift, self.size)

    def greet(self, barrier):
        for shift in range(1, self.size):
            pl.semaphore_signal(
                barrier, inc=1, device_id={self.axis: self.peer(shift)}, device_id_type=MESH
            )
        return self.size - 1

    def copy(self, shift, arriving):
        landing = self.peer(self.size - shift) if arriving else self.index
        return pltpu.make_async_remote_copy(
            src_ref=self.block.at[self.peer(shift)],
            dst_ref=self.out.at[landing],
            send_sem=self.send.at[shift],
            recv_sem=self.recv.at[shift],
            device_id={self.axis: self.peer(shift)},
            device_id_type=MESH,
        )

    def begin(self):
        pltpu.make_async_copy(
            self.block.at[self.index], self.out.at[self.index], self.local.at[0]
        ).start()
        for shift in range(1, self.size):
            self.copy(shift, False).start()

    def steps(self):
        return 0

    def advance(self, step):
        pass

    def finish(self):
        for shift in range(1, self.size):
            self.copy(shift, False).wait_send()
            self.copy(shift, True).wait_recv()
        pltpu.make_async_copy(
            self.block.at[self.index], self.out.at[self.index], self.local.at[0]
        ).wait()


class Halo:
    def __init__(self, axis, size, block, out, send, recv):
        self.axis, self.size, self.block, self.out = axis, size, block, out
        self.send, self.recv = send, recv
        self.index = lax.axis_index(axis)
        self.above, self.below = self.index > 0, self.index < size - 1

    def greet(self, barrier):
        for present, target in ((self.above, self.index - 1), (self.below, self.index + 1)):

            @pl.when(present)
            def _():
                pl.semaphore_signal(
                    barrier, inc=1, device_id={self.axis: target}, device_id_type=MESH
                )

        return jnp.where(self.above, 1, 0) + jnp.where(self.below, 1, 0)

    def copy(self, side):
        return pltpu.make_async_remote_copy(
            src_ref=self.block.at[side],
            dst_ref=self.out.at[1 - side],
            send_sem=self.send.at[side],
            recv_sem=self.recv.at[side],
            device_id={self.axis: self.index - 1 + 2 * side},
            device_id_type=MESH,
        )

    def begin(self):
        for side, present in ((0, self.above), (1, self.below)):

            @pl.when(present)
            def _():
                self.copy(side).start()

            @pl.when(jnp.logical_not(present))
            def _():
                self.out[side] = jnp.zeros(self.out.shape[1:], self.out.dtype)

    def steps(self):
        return 0

    def finish(self):
        for side, present in ((0, self.above), (1, self.below)):

            @pl.when(present)
            def _():
                self.copy(side).wait_send()
                self.copy(1 - side).wait_recv()


class Swap:
    def __init__(self, axis, size, block, out, send, recv, local):
        self.axis, self.block, self.out = axis, block, out
        self.send, self.recv, self.local = send, recv, local
        self.index = lax.axis_index(axis)
        self.parity = lax.rem(self.index, 2)

    def copy(self, arriving):
        return pltpu.make_async_remote_copy(
            src_ref=self.block,
            dst_ref=self.out.at[1 - self.parity if arriving else self.parity],
            send_sem=self.send.at[0],
            recv_sem=self.recv.at[0],
            device_id={self.axis: self.index + 1 - 2 * self.parity},
            device_id_type=MESH,
        )

    def begin(self):
        pltpu.make_async_copy(self.block, self.out.at[self.parity], self.local.at[0]).start()
        self.copy(False).start()

    def steps(self):
        return 0

    def finish(self):
        self.copy(False).wait_send()
        self.copy(True).wait_recv()
        pltpu.make_async_copy(self.block, self.out.at[self.parity], self.local.at[0]).wait()


def line_scratch(size, paired):
    dma = pltpu.SemaphoreType.DMA
    length = size // 2 if paired else size
    steps = max(length - 1, 1)
    scratch = [dma((2, steps)), dma((2, steps)), dma((1,))]
    if paired:
        scratch += [dma((2 * length,)), dma((2 * length,))]
    return scratch


def run_flows(flows):
    for flow in flows:
        flow.begin()
    for step in range(max(flow.steps() for flow in flows)):
        for flow in flows:
            if step < flow.steps():
                flow.advance(step)
    for flow in flows:
        flow.finish()


def move_kernel(kinds, *refs):
    count = len(kinds)
    blocks, outs, sems = refs[:count], refs[count : 2 * count], list(refs[2 * count :])
    flows, leaders = [], {}

    def take(number):
        taken = sems[:number]
        del sems[:number]
        return taken

    for (kind, axis, size, chunks), block, out in zip(kinds, blocks, outs):
        if kind == "exchange":
            flow = Exchange(axis, size, block, out, *take(3))
            leaders[axis] = flow
            flows.append(flow)
        elif kind == "halo":
            flows.append(Halo(axis, size, block, out, *take(2)))
        elif kind == "swap":
            flows.append(Swap(axis, size, block, out, *take(3)))
        else:
            paired = kind == "paired"
            rows = block.shape[0] // chunks
            for chunk in range(chunks):
                part = pl.ds(chunk * rows, rows)
                flow = Line(
                    axis, size, paired, block.at[part], ChunkedOut(out, part),
                    *take(5 if paired else 3), *(() if paired else (None, None)),
                )
                flows.append(flow)
        leaders.setdefault(axis, flows[-1])
    barrier = pltpu.get_barrier_semaphore()
    expected = 0
    for flow in leaders.values():
        expected = expected + flow.greet(barrier)
    pl.semaphore_wait(barrier, expected)
    run_flows(flows)


class ChunkedOut:
    def __init__(self, out, part):
        self.out, self.part = out, part

    @property
    def at(self):
        return self

    def __getitem__(self, slot):
        return self.out.at[slot, self.part]


def move(identity, items):
    kinds, arrays, shapes, scratch = [], [], [], []
    sent = 0
    for kind, axis, array, chunks in items:
        size = lax.axis_size(axis)
        kinds.append((kind, axis, size, chunks))
        arrays.append(array)
        lead = {"exchange": (), "halo": (), "swap": (2,)}.get(kind, (size,))
        shapes.append(jax.ShapeDtypeStruct(lead + array.shape, array.dtype))
        sent += array.size * array.dtype.itemsize
        dma = pltpu.SemaphoreType.DMA
        if kind == "exchange":
            scratch += [dma((size,)), dma((size,)), dma((1,))]
        elif kind == "halo":
            scratch += [dma((2,)), dma((2,))]
        elif kind == "swap":
            scratch += [dma((1,)), dma((1,)), dma((1,))]
        else:
            scratch += line_scratch(size, kind == "paired") * chunks
    return pl.pallas_call(
        functools.partial(move_kernel, tuple(kinds)),
        out_shape=tuple(shapes),
        in_specs=[pl.BlockSpec(memory_space=pltpu.VMEM)] * len(arrays),
        out_specs=tuple([pl.BlockSpec(memory_space=pltpu.VMEM)] * len(arrays)),
        scratch_shapes=scratch,
        compiler_params=pltpu.CompilerParams(
            collective_id=identity, has_side_effects=True, vmem_limit_bytes=VMEM_LIMIT
        ),
        cost_estimate=pl.CostEstimate(flops=0, bytes_accessed=30 * sent, transcendentals=0),
        name=f"move{identity}",
    )(*arrays)


def close_kernel(
    axis, size, row_axis, row_size, part_ref, act_ref, project_ref, token_ref, rows_ref,
    came_ref, block_ref, send, recv, local, *line_sems,
):
    line = Line(row_axis, row_size, True, block_ref, rows_ref, *line_sems)
    swap = Exchange(axis, size, part_ref, came_ref, send, recv, local)
    barrier = pltpu.get_barrier_semaphore()
    expected = line.greet(barrier) + swap.greet(barrier)
    pl.semaphore_wait(barrier, expected)
    swap.begin()
    swap.finish()
    total = act_ref[...].astype(jnp.float32)
    for origin in range(size):
        total = total + came_ref[origin].astype(jnp.float32)
    token = total.astype(jnp.bfloat16)
    token_ref[...] = token
    block_ref[...] = matmul(token, project_ref[...]).astype(jnp.bfloat16)
    run_flows([line])


def close(identity, axis, row_axis, parts, act_rows, project):
    size, row_size = lax.axis_size(axis), lax.axis_size(row_axis)
    rows, depth = act_rows.shape
    dma = pltpu.SemaphoreType.DMA
    vmem = pl.BlockSpec(memory_space=pltpu.VMEM)
    return pl.pallas_call(
        functools.partial(close_kernel, axis, size, row_axis, row_size),
        out_shape=(
            jax.ShapeDtypeStruct((rows, depth), jnp.bfloat16),
            jax.ShapeDtypeStruct((row_size, rows, project.shape[1]), jnp.bfloat16),
        ),
        in_specs=[vmem] * 3,
        out_specs=(vmem, vmem),
        scratch_shapes=[
            pltpu.VMEM(parts.shape, jnp.bfloat16),
            pltpu.VMEM((rows, project.shape[1]), jnp.bfloat16),
            dma((size,)),
            dma((size,)),
            dma((1,)),
        ]
        + line_scratch(row_size, True),
        compiler_params=pltpu.CompilerParams(
            collective_id=identity, has_side_effects=True, vmem_limit_bytes=VMEM_LIMIT
        ),
        name="close",
    )(parts, act_rows, project)


def attention_kernel(heads, span, q_ref, gate_ref, kv_ref, bias_ref, mask_ref, out_ref):
    rows, width = q_ref.shape[1], q_ref.shape[2]
    pieces, piece_rows = kv_ref.shape[0], kv_ref.shape[2]
    queries = q_ref[0]
    head_of = lax.broadcasted_iota(jnp.int32, (rows, width), 1) // HD
    stacked = jnp.concatenate(
        [jnp.where(head_of == head, queries, 0).astype(jnp.bfloat16) for head in range(heads)], axis=0
    )
    scale = 1.0 / math.sqrt(HD)
    maxima = totals = summed = None
    for first in range(0, pieces, span):
        taken = min(span, pieces - first)
        keys = jnp.concatenate([kv_ref[first + i, 0, :, :width] for i in range(taken)], axis=0)
        values = jnp.concatenate([kv_ref[first + i, 0, :, width:] for i in range(taken)], axis=0)
        columns = pl.ds(first * piece_rows, taken * piece_rows)
        scores = (
            lax.dot_general(
                stacked, keys, (((1,), (1,)), ((), ())), preferred_element_type=jnp.float32
            )
            * scale
        )
        bias = bias_ref[:, :, columns].reshape(heads * rows, taken * piece_rows)
        scores = scores + bias.astype(jnp.float32)
        scores = jnp.where(mask_ref[:, columns] > 0, scores, FAR)
        block_max = jnp.max(scores, axis=-1, keepdims=True)
        new_maxima = block_max if maxima is None else jnp.maximum(maxima, block_max)
        weights = jnp.exp(scores - new_maxima)
        block_total = jnp.sum(weights, axis=-1, keepdims=True)
        update = matmul(weights.astype(jnp.bfloat16), values)
        if maxima is None:
            totals, summed = block_total, update
        else:
            factor = jnp.exp(maxima - new_maxima)
            totals = totals * factor + block_total
            summed = summed * factor + update
        maxima = new_maxima
    attended = summed / totals
    result = jnp.zeros((rows, width), jnp.float32)
    for head in range(heads):
        result = result + jnp.where(head_of == head, attended[head * rows : (head + 1) * rows], 0.0)
    gate = jax.nn.sigmoid(gate_ref[0].astype(jnp.float32))
    out_ref[0] = (result * gate).astype(jnp.bfloat16)


def token_attention(query_rows, gate_rows, kv_all, pair_bias, mask_row):
    groups, rows, width = query_rows.shape
    heads, keys = pair_bias.shape[0], pair_bias.shape[2]
    pieces, piece_rows = kv_all.shape[0], kv_all.shape[2]
    one = lambda g: (g, 0, 0)
    return pl.pallas_call(
        functools.partial(attention_kernel, heads, max(512 // piece_rows, 1)),
        grid=(groups,),
        in_specs=[
            pl.BlockSpec((1, rows, width), one),
            pl.BlockSpec((1, rows, width), one),
            pl.BlockSpec((pieces, 1, piece_rows, 2 * width), lambda g: (0, g, 0, 0)),
            pl.BlockSpec((heads, rows, keys), lambda g: (0, 0, 0)),
            pl.BlockSpec((1, keys), lambda g: (0, 0)),
        ],
        out_specs=pl.BlockSpec((1, rows, width), one),
        out_shape=jax.ShapeDtypeStruct((groups, rows, width), jnp.bfloat16),
        compiler_params=pltpu.CompilerParams(vmem_limit_bytes=VMEM_LIMIT),
        name="token_attention",
    )(query_rows, gate_rows, kv_all, pair_bias, mask_row)


def atom_kernel(
    first_ref, bounds_ref, rows_ref, skip_ref, cond_ref, rim_ref, token_ref, weight_ref, vector_ref,
    position_ref, bias_ref, out_ref, state_ref, query_ref, gate_ref, key_ref, value_ref, held_ref,
):
    count, channels = query_ref.shape
    head_width = channels // HA
    tokens = rows_ref.shape[0]
    chunk = min(512, tokens)
    inner = pl.ds(RIM, count)
    owners = token_ref[...]
    taken = jnp.zeros((owners.shape[0], channels), jnp.float32)
    for start in range(0, tokens, chunk):
        column = lax.broadcasted_iota(jnp.int32, (owners.shape[0], chunk), 1) + start
        hit = jnp.where(owners == column, 1.0, 0.0).astype(jnp.bfloat16)
        taken = taken + matmul(hit, rows_ref[start : start + chunk, :])
    skip = jnp.concatenate([rim_ref[0, :, :channels], skip_ref[...], rim_ref[1, :, :channels]], axis=0)
    cond = jnp.concatenate([rim_ref[0, :, channels:], cond_ref[...], rim_ref[1, :, channels:]], axis=0)
    state = skip.astype(jnp.float32) + taken
    state_ref[...] = state
    normed = layer_norm(cond).astype(jnp.bfloat16)
    atom_x = (
        jax.nn.sigmoid(matmul(normed, weight_ref[0]) + vector_ref[0:1, :]) * layer_norm(state)
        + matmul(normed, weight_ref[1])
    ).astype(jnp.bfloat16)
    own_x = atom_x[RIM : RIM + count, :]
    query_ref[...] = (matmul(own_x, weight_ref[2]) + vector_ref[1:2, :]).astype(jnp.bfloat16)
    gate_ref[...] = matmul(own_x, weight_ref[5]).astype(jnp.bfloat16)
    key_ref[...] = matmul(atom_x, weight_ref[3]).astype(jnp.bfloat16)
    value_ref[...] = matmul(atom_x, weight_ref[4]).astype(jnp.bfloat16)
    head_of = lax.broadcasted_iota(jnp.int32, (WQ, channels), 1) // head_width
    lane = lax.broadcasted_iota(jnp.int32, (1, WK), 1)
    scale = 1.0 / math.sqrt(head_width)

    def windows(step, carry):
        scores = []
        bases = [pl.multiple_of(step * (BATCH * WQ) + i * WQ, WQ) for i in range(BATCH)]
        for i, base in enumerate(bases):
            queries = query_ref[pl.ds(base, WQ), :]
            stacked = jnp.concatenate(
                [jnp.where(head_of == head, queries, 0).astype(jnp.bfloat16) for head in range(HA)],
                axis=0,
            )
            score = lax.dot_general(
                stacked, key_ref[pl.ds(base, WK), :], (((1,), (1,)), ((), ())),
                preferred_element_type=jnp.float32,
            )
            bias = bias_ref[:, pl.ds(base, WQ), :].reshape(HA * WQ, WK).astype(jnp.float32)
            slot = first_ref[0] + base - RIM + lane
            index = step * BATCH + i
            inside = (slot >= bounds_ref[2 * index]) & (slot < bounds_ref[2 * index + 1])
            scores.append(jnp.where(inside, score * scale + bias, FAR))
        weights = [jnp.exp(score - jnp.max(score, axis=-1, keepdims=True)) for score in scores]
        results = []
        for base, weight in zip(bases, weights):
            attended = matmul(weight.astype(jnp.bfloat16), value_ref[pl.ds(base, WK), :])
            attended = attended / jnp.sum(weight, axis=-1, keepdims=True)
            result = jnp.zeros((WQ, channels), jnp.float32)
            for head in range(HA):
                result = result + jnp.where(
                    head_of == head, attended[head * WQ : (head + 1) * WQ], 0.0
                )
            results.append(result)
        start = pl.multiple_of(step * (BATCH * WQ), BATCH * WQ)
        held_ref[pl.ds(start, BATCH * WQ), :] = jnp.concatenate(results, axis=0)
        return carry

    lax.fori_loop(0, count // (BATCH * WQ), windows, 0)
    gated = (held_ref[...] * jax.nn.sigmoid(gate_ref[...].astype(jnp.float32))).astype(jnp.bfloat16)
    fresh = state_ref[inner, :] + matmul(gated, weight_ref[6])
    final = layer_norm(fresh).astype(jnp.bfloat16)
    out_ref[...] = lax.dot_general(
        position_ref[...], final, (((1,), (1,)), ((), ())), preferred_element_type=jnp.float32
    )


BATCH = 8


def atom_block(first, bounds, rows, skip, cond, rims, owners, weights, vectors, positions, bias):
    count, channels = bias.shape[1], skip.shape[1]
    extended = skip.shape[0] + 2 * RIM
    smem = pl.BlockSpec(memory_space=pltpu.SMEM)
    vmem = pl.BlockSpec(memory_space=pltpu.VMEM)
    return pl.pallas_call(
        atom_kernel,
        in_specs=[smem, smem] + [vmem] * 9,
        out_specs=vmem,
        out_shape=jax.ShapeDtypeStruct((positions.shape[0], count), jnp.float32),
        scratch_shapes=[
            pltpu.VMEM((extended, channels), jnp.float32),
            pltpu.VMEM((count, channels), jnp.bfloat16),
            pltpu.VMEM((count, channels), jnp.bfloat16),
            pltpu.VMEM((extended, channels), jnp.bfloat16),
            pltpu.VMEM((extended, channels), jnp.bfloat16),
            pltpu.VMEM((count, channels), jnp.float32),
        ],
        compiler_params=pltpu.CompilerParams(vmem_limit_bytes=VMEM_LIMIT),
        name="atom_block",
    )(first, bounds, rows, skip, cond, rims, owners, weights, vectors, positions, bias)


def rims(array):
    return jnp.stack([array[:RIM], array[array.shape[0] - RIM :]])


def per_device(
    token_act,
    token_cond,
    pair_bias,
    token_mask,
    ada_weights,
    attention_in,
    attention_out,
    transition_in,
    transition_out,
    token_vectors,
    atom_skip,
    atom_cond,
    atom_bias,
    window_bounds,
    atom_token,
    atom_weights,
    token_to_atom,
    atom_vectors,
    position_out,
):
    groups = lax.axis_size("fsdp")
    act_rows = token_act[0]
    row_count, depth = act_rows.shape
    column_count = attention_in.shape[2]
    channels = atom_cond.shape[1]
    start = lax.axis_index("fsdp") * column_count
    atom_rims = rims(jnp.concatenate([atom_skip[0], atom_cond], axis=1))
    owner_rims = jnp.pad(rims(atom_token)[:, None, :], ((0, 0), (0, 0), (0, 2 * WK - RIM)))
    small = jnp.concatenate([atom_weights.reshape(-1, channels), token_to_atom], axis=0)
    small_height = small.shape[0] // 2
    small_half = lax.dynamic_slice_in_dim(
        small, lax.rem(lax.axis_index("seq"), 2) * small_height, small_height
    )

    cond_normed = layer_norm(token_cond[0]).astype(jnp.bfloat16)
    act_normed = layer_norm(act_rows).astype(jnp.bfloat16)
    act_slots = jnp.transpose(act_normed.reshape(row_count, groups, column_count), (1, 0, 2))
    cond_all, act_all, atom_rims, owner_rims = move(
        1,
        (
            ("line", "fsdp", cond_normed, 4),
            ("exchange", "fsdp", pack(act_slots), 1),
            ("halo", "seq", atom_rims, 1),
            ("halo", "seq", owner_rims, 1),
        ),
    )
    owners = jnp.concatenate([owner_rims[0, 0, :RIM], atom_token, owner_rims[1, 0, :RIM]])[:, None]
    cond_flat = cond_all.reshape(groups * row_count, depth)
    act_flat = unpack(act_all).reshape(groups * row_count, column_count).astype(jnp.float32)

    def adaptive(scale_index, shift_index, vector_index):
        offset = lax.dynamic_slice_in_dim(token_vectors[vector_index], start, column_count)
        scaled = jax.nn.sigmoid(matmul(cond_flat, ada_weights[scale_index]) + offset) * act_flat
        rows = (scaled + matmul(cond_flat, ada_weights[shift_index])).astype(jnp.bfloat16)
        return pack(rows.reshape(groups, row_count, column_count))

    def joined(array):
        array = unpack(array)
        return jnp.transpose(array, (1, 2, 0, 3)).reshape(groups * row_count, depth)

    attend_all, small_halves = move(
        2, (("line", "fsdp", adaptive(0, 1, 0), groups), ("line", "fsdp", small_half, 1))
    )
    transit_part = adaptive(2, 3, 1)
    attend_flat = joined(attend_all)
    query_bias = lax.dynamic_slice_in_dim(token_vectors[2], start, column_count)

    def project(index):
        return matmul(attend_flat, attention_in[index])

    def grouped(array):
        return array.astype(jnp.bfloat16).reshape(groups, row_count, -1)

    keys_values = jnp.concatenate([grouped(project(1)), grouped(project(2))], axis=-1)
    kv_all, transit_all, mask_all, small_all = move(
        3,
        (
            ("paired", "seq", keys_values, groups),
            ("line", "fsdp", transit_part, groups),
            ("paired", "seq", token_mask[None], 1),
            ("swap", "seq", small_halves, 1),
        ),
    )
    small_all = jnp.transpose(small_all, (1, 0, 2, 3)).reshape(groups, -1, channels)
    query_rows = grouped(project(0) + query_bias)
    gate_rows = grouped(project(3))
    weight_rows = atom_weights.size // channels
    atom_full = jnp.transpose(
        small_all[:, :weight_rows].reshape((groups,) + atom_weights.shape), (1, 2, 0, 3)
    ).reshape(atom_weights.shape[0], channels, channels)
    project_full = small_all[:, weight_rows:].reshape(depth, channels)
    gated = token_attention(
        query_rows, gate_rows, kv_all, pair_bias, mask_all.reshape(1, -1)
    ).reshape(groups * row_count, -1)
    transit_flat = joined(transit_all)
    hidden = (
        jax.nn.silu(matmul(transit_flat, transition_in[0])) * matmul(transit_flat, transition_in[1])
    ).astype(jnp.bfloat16)
    partial_sum = matmul(gated, attention_out) + matmul(hidden, transition_out)
    token_result, all_rows = close(
        4,
        "fsdp",
        "seq",
        partial_sum.astype(jnp.bfloat16).reshape(groups, row_count, depth),
        act_rows,
        project_full,
    )
    first_atom = (lax.axis_index("seq") * atom_cond.shape[0]).astype(jnp.int32).reshape(1)
    update = atom_block(
        first_atom,
        window_bounds.reshape(-1),
        all_rows.reshape(-1, channels),
        atom_skip[0],
        atom_cond,
        atom_rims,
        owners,
        atom_full,
        atom_vectors,
        position_out,
        atom_bias,
    )
    return (token_result[None], update[None])


def solution(mesh):
    in_specs = (
        P(("sample", "fsdp"), "seq", None),
        P(("sample", "fsdp"), "seq", None),
        P("fsdp", "seq", None),
        P("seq"),
        P(None, None, "fsdp"),
        P(None, None, "fsdp"),
        P("fsdp", None),
        P(None, None, "fsdp"),
        P("fsdp", None),
        P(),
        P(("sample", "fsdp"), "seq", None),
        P("seq", None),
        P(None, "seq", None),
        P("seq", None),
        P("seq"),
        P(None, None, "fsdp"),
        P("fsdp", None),
        P(),
        P(),
    )
    out_specs = (P(("sample", "fsdp"), "seq", None), P(("sample", "fsdp"), None, "seq"))
    return jax.shard_map(
        per_device, mesh=mesh, in_specs=in_specs, out_specs=out_specs, check_vma=False
    )
```
